32 devices in a mesh: gx: 2 (over y), gy: 4 (over z), gz: 4 (over x, core).
Axes of the slice: x: 2, y: 2, z: 4, core: 2. Of those that a mesh axis runs over, the one named last changes fastest.
Arguments:
- tokens: bfloat16 [512, 6144], P(('gx', 'gy'), 'gz'), may hold values from -6 to 6
- grad_out: bfloat16 [512, 6144], P(('gx', 'gy'), 'gz'), may hold values from -1.5 to 1.5
- w_in: bfloat16 [6144, 12288], P('gz', ('gy', 'gx')), may hold values from -0.078125 to 0.078125
- w_out: bfloat16 [12288, 6144], P(('gy', 'gx'), 'gz'), may hold values from -0.0546875 to 0.0546875
Outputs:
- mlp_out: bfloat16 [512, 6144], P(('gx', 'gy'), 'gz')
- tok_grad: bfloat16 [512, 6144], P(('gx', 'gy'), 'gz')
- win_grad: float32 [6144, 12288], P('gz', ('gy', 'gx'))
- wout_grad: float32 [12288, 6144], P(('gy', 'gx'), 'gz')
The draws below stay inside these ranges and needn't reach their ends.
All inputs are finite; a program needn't handle non-finite values.
Results may differ from the reference program's by a relative error of at most 0.01.
Values may be sent and summed in bfloat16 or wider, within the bound.
A program may use at most 128 MiB of HBM per device.

```python
import math
import jax
import jax.numpy as jnp
from jax import lax

D = 6144
FF = 12288
ROWS = 256
TOKENS = 512
N_GX = 2


def shard_levels(own_key, dims, shards, least, high):
    factor_of, own = 1.0, jax.random.fold_in(own_key, 6)
    for position, parts in shards:
        draws = jnp.exp(jax.random.uniform(jax.random.fold_in(own, position), (parts,), jnp.float32, least / len(shards), high / len(shards)))
        factor_of = factor_of * jnp.repeat(draws, dims[position] // parts).reshape([-1 if axis == position else 1 for axis in range(len(dims))])
    return factor_of


def centred(own_key, dims, spread, bound, shards=(), held_as=jnp.bfloat16):
    array = spread * jax.random.normal(own_key, dims, jnp.float32)
    if shards:
        array = array * shard_levels(own_key, dims, shards, -0.22, 0.18)
    return jnp.clip(array, -bound, bound).astype(held_as)


def setup_inputs(seed: int = 0) -> dict:
    keys = jax.random.split(jax.random.key(seed), 5)
    tokens = centred(keys[0], (TOKENS, D), 1.0, 6.0, ((0, 8), (1, 4)))
    grad_out = centred(keys[1], (TOKENS, D), 0.25, 1.5, ((0, 8), (1, 4)))
    w_in = centred(keys[2], (D, FF), D ** -0.5, 0.078125, ((0, 4), (1, 8)))
    w_out = centred(keys[3], (FF, D), FF ** -0.5, 0.0546875, ((0, 8), (1, 4)))
    return {"tokens": tokens, "grad_out": grad_out, "w_in": w_in, "w_out": w_out}


def gelu_slope(values):
    cdf = 0.5 * (1.0 + jax.scipy.special.erf(values * 0.7071067811865476))
    density = jnp.exp(-0.5 * values * values) * 0.3989422804014327
    return cdf + values * density

def reference(tokens, grad_out, w_in, w_out):
    block_scale = 1.0 / math.sqrt(ROWS)
    pre = jnp.dot(tokens, w_in, preferred_element_type=jnp.float32)
    act = jax.nn.gelu(pre, approximate=False).astype(jnp.bfloat16)
    mlp_out = jnp.dot(act, w_out, preferred_element_type=jnp.float32).astype(jnp.bfloat16)
    d_act = jnp.dot(grad_out, w_out.T, preferred_element_type=jnp.float32)
    d_pre = (d_act * gelu_slope(pre)).astype(jnp.bfloat16)
    tok_grad = jnp.dot(d_pre, w_in.T, preferred_element_type=jnp.float32).astype(jnp.bfloat16)
    wout_grad = jnp.zeros((FF, D), jnp.float32)
    win_grad = jnp.zeros((D, FF), jnp.float32)
    for block in range(N_GX):
        lower = block * ROWS
        part_out = (jnp.dot(act[lower:lower + ROWS].T, grad_out[lower:lower + ROWS], preferred_element_type=jnp.float32) * block_scale).astype(jnp.bfloat16)
        part_in = (jnp.dot(tokens[lower:lower + ROWS].T, d_pre[lower:lower + ROWS], preferred_element_type=jnp.float32) * block_scale).astype(jnp.bfloat16)
        part_out = lax.optimization_barrier(part_out)
        part_in = lax.optimization_barrier(part_in)
        wout_grad = wout_grad + part_out.astype(jnp.float32)
        win_grad = win_grad + part_in.astype(jnp.float32)
    return (mlp_out, tok_grad, win_grad, wout_grad)
```

```python
import functools
import math

import jax
import jax.numpy as jnp
from jax import lax
from jax.experimental import pallas as pl
from jax.experimental.pallas import tpu as pltpu
from jax.sharding import PartitionSpec as P

MESH = pl.DeviceIdType.MESH
F32, BF16 = jnp.float32, jnp.bfloat16

GATHER_VIA = (True, False)
REDUCE_VIA = (True, False)
PIECES = 2
CHUNKS = 2


def contract(left, right, dims):
    return lax.dot_general(left, right, (dims, ((), ())), preferred_element_type=F32)


def order_table(ny):
    centre = (ny - 1) / 2
    return [
        sorted(range(ny), key=lambda k: (abs(k - z), abs(k - centre))) for z in range(ny)
    ]


def schedule(ny):
    last = ny - 1
    steps = [("Fo", 0, 0), ("Fy", 1, 0), ("Fo", 0, 1), ("Fc", 0, 0), ("Fz", 1, 0), ("P", 0, 0)]
    steps += [("Fo", 0, 2), ("J", 0, 0), ("Fc", 0, 1), ("P", 0, 1), ("Fo", 1, 1), ("Fc", 1, 0)]
    steps += [("Fo", 0, 3), ("J", 0, 1), ("Fc", 0, 2), ("P", 0, 2), ("G", 0, 0), ("J", 0, 2)]
    steps += [("P", 1, 0), ("Fo", 1, 2), ("Fc", 0, 3), ("P", 0, 3), ("J", 1, 0), ("G", 0, 1), ("J", 0, 3)]
    steps += [("E", 0, 0), ("Fc", 1, 1), ("P", 1, 1), ("Fo", 1, 3), ("G", 0, 2), ("J", 1, 1)]
    steps += [("E", 0, 1), ("Fc", 1, 2), ("P", 1, 2), ("G", 0, 3), ("J", 1, 2), ("G", 1, 0)]
    steps += [("E", 0, 2), ("E", 0, 3), ("Fc", 1, 3), ("P", 1, 3), ("S", 0, 0), ("G", 1, 1), ("J", 1, 3)]
    steps += [("X", 0, 0), ("E", 1, 0), ("R", 0, 3), ("E", 1, 1), ("R", 0, 2), ("G", 1, 2), ("E", 1, 2)]
    steps += [("R", 0, 1), ("G", 1, 3), ("E", 1, 3), ("S", 1, 0), ("X", 1, 0), ("R", 0, 0)]
    steps += [("R", 1, 3), ("R", 1, 2), ("R", 1, 1), ("R", 1, 0)]
    return steps


def simple_schedule(ny):
    steps = []
    for arr in range(2):
        steps += [("Fo", arr, i) for i in range(ny)] if arr == 0 else [("Fy", 1, 0), ("Fz", 1, 0)]
        if arr == 1:
            steps += [("Fo", arr, i) for i in range(1, ny)]
        steps += [("Fc", arr, i) for i in range(ny)]
        for name in "PJGE":
            steps += [(name, arr, i) for i in range(ny)]
        steps += [("S", arr, 0), ("X", arr, 0)]
    for arr in range(2):
        steps += [("R", arr, i) for i in reversed(range(ny))]
    return steps


def ring_kernel(
    nx, ny, nz,
    tok_ref, grad_ref, win_ref, wout_ref,
    mlp_ref, tgrad_ref, tok_out, grad_out, act_out, dpre_out,
    rows_all, win, wout, part, pair_in, paired, part_in, slope, hid,
    mine_sum, cross, y_in, z_in, v_in, fold,
    local, a_y, a_z, a_v, p_sem, b_sem, c_sem, d_y, d_z, d_v,
):
    x, y, z = lax.axis_index("gx"), lax.axis_index("gy"), lax.axis_index("gz")
    t, width = tok_ref.shape
    hidden = win_ref.shape[1]
    rows = nx * t
    share = rows // 2
    half = nz // 2
    chunks = CHUNKS if hidden % (128 * CHUNKS) == 0 else 1
    core, chip = lax.rem(z, 2), lax.div(z, 2)
    partner = z + 1 - 2 * core
    sends = []

    def pick(values):
        total = 0
        for at, value in enumerate(values):
            total = total + jnp.where(y == at, value, 0)
        return total

    table = order_table(ny)
    near = [pick([table[at][i] for at in range(ny)]) for i in range(ny)]
    gap = [pick([abs(table[at][i] - at) for at in range(ny)]) for i in range(ny)]
    gaps = [{abs(table[at][i] - at) for at in range(ny)} for i in range(ny)]
    heading = [jnp.where(near[i] < y, 0, 1) for i in range(ny)]
    step_of = [1 - 2 * heading[i] for i in range(ny)]
    beyond = [
        jnp.logical_or(
            jnp.logical_and(near[i] < y, y < ny - 1), jnp.logical_and(near[i] > y, y > 0)
        )
        for i in range(ny)
    ]
    has_up, has_down = y < ny - 1, y > 0

    def via(flags, arr, i):
        if not flags[arr] or i == 0 or 1 not in gaps[i]:
            return False
        if gaps[i] == {1}:
            return True
        return gap[i] == 1

    def when(pred, body):
        if pred is True:
            body()
        elif pred is not False:
            pl.when(pred)(body)

    def negate(pred):
        return (not pred) if isinstance(pred, bool) else jnp.logical_not(pred)

    def remote(src, dst, sems, index, device):
        return pltpu.make_async_remote_copy(
            src_ref=src, dst_ref=dst, send_sem=sems.at[(0, *index)],
            recv_sem=sems.at[(1, *index)], device_id=device, device_id_type=MESH,
        )

    def send(src, dst, sems, index, device, pred=True):
        if pred is False:
            return
        copy = remote(src, dst, sems, index, device)
        when(pred, copy.start)
        sends.append((pred, copy))

    def arrive(ref, sems, index):
        remote(ref, ref, sems, index, {"gz": z}).wait_recv()

    def peer(e):
        return {"gx": lax.rem(x + e, nx)}

    def piece(p):
        return pl.ds(p * (width // PIECES), width // PIECES)

    def chunk(c):
        return pl.ds(c * (hidden // chunks), hidden // chunks)

    def tiles(size, body, base=0):
        tile = 256 if size % 256 == 0 else 128

        def step(i, carry):
            body(pl.ds(pl.multiple_of(base + i * tile, 128), tile))
            return carry

        lax.fori_loop(0, size // tile, step, 0)

    stage = [
        pltpu.make_async_copy(tok_ref, rows_all.at[0, y, 0], local.at[0]),
        pltpu.make_async_copy(grad_ref, rows_all.at[1, y, 0], local.at[1]),
        pltpu.make_async_copy(win_ref, win, local.at[2]),
        pltpu.make_async_copy(wout_ref, wout, local.at[3]),
    ]
    for copy in stage:
        copy.start()
    barrier = pltpu.get_barrier_semaphore()
    for name, me, n in (("gx", x, nx), ("gy", y, ny), ("gz", z, nz)):
        for d in range(1, n):
            pl.semaphore_signal(
                barrier, inc=1, device_id={name: lax.rem(me + d, n)}, device_id_type=MESH
            )
    pl.semaphore_wait(barrier, nx + ny + nz - 3)
    stores = []

    def to_columns(arr, i, p, pred=True):
        block = rows_all.at[arr, near[i], 0, :, piece(p)]
        for e in range(1, nx):
            dst = rows_all.at[arr, near[i], nx - e, :, piece(p)]
            send(block, dst, a_y, (arr, i, nx - e, p), peer(e), pred)

    def own_columns(arr):
        stage[arr].wait()
        for p in range(PIECES):
            to_columns(arr, 0, p)

    def own_line(arr):
        for p in range(PIECES):
            block = rows_all.at[arr, y, 0, :, piece(p)]
            send(block, block, a_z, (arr, 0, y, p), {"gy": y + 1}, has_up)
            send(block, block, a_z, (arr, 1, y, p), {"gy": y - 1}, has_down)

    def own_column(arr, i):
        if i == 0:
            own_columns(arr)
            own_line(arr)
            return
        for p in range(PIECES):
            block = rows_all.at[arr, near[i], 0, :, piece(p)]
            arrive(block, a_z, (arr, heading[i], near[i], p))
            send(
                block, block, a_z, (arr, heading[i], near[i], p),
                {"gy": y + step_of[i]}, beyond[i],
            )
            to_columns(arr, i, p, negate(via(GATHER_VIA, arr, i)))

    def other_columns(arr, i):
        by_line = via(GATHER_VIA, arr, i)
        for p in range(PIECES):
            for e in range(1, nx):
                block = rows_all.at[arr, near[i], e, :, piece(p)]
                when(by_line, lambda: arrive(block, a_v, (arr, heading[i], e, p)))
                when(negate(by_line), lambda: arrive(block, a_y, (arr, i, e, p)))
                if i == 0 and GATHER_VIA[arr]:
                    send(block, block, a_v, (arr, 0, e, p), {"gy": y + 1}, has_up)
                    send(block, block, a_v, (arr, 1, e, p), {"gy": y - 1}, has_down)

    def project(arr, i):
        if i == 0:
            stage[2 + arr].wait()
        left = rows_all.at[arr, near[i]]

        def body(cols):
            lhs = left[...].reshape(rows, width)
            if arr == 0:
                out = contract(lhs, win[:, cols], ((1,), (0,)))
            else:
                out = contract(lhs, wout[cols, :], ((1,), (1,)))
            part[arr, i, :, :, cols] = out.astype(BF16).reshape(2, share, -1)

        for c in range(chunks):
            tiles(hidden // chunks, body, c * (hidden // chunks))
            send(
                part.at[arr, i, 1 - core, :, chunk(c)], pair_in.at[arr, i, :, chunk(c)],
                p_sem, (arr, i, c), {"gz": partner},
            )

    def join(arr, i):
        def body(cols):
            total = part[arr, i, core, :, cols].astype(F32)
            total = total + pair_in[arr, i, :, cols].astype(F32)
            paired[arr, i, :, cols] = total.astype(BF16)

        for c in range(chunks):
            arrive(pair_in.at[arr, i, :, chunk(c)], p_sem, (arr, i, c))
            tiles(hidden // chunks, body, c * (hidden // chunks))
            for d in range(1, half):
                to = lax.rem(chip + d, half)
                send(
                    paired.at[arr, i, :, chunk(c)], part_in.at[arr, i, d, :, chunk(c)],
                    b_sem, (arr, i, d, c), {"gz": 2 * to + core},
                )

    def activate(arr, i):
        def body(cols):
            total = paired[arr, i, :, cols].astype(F32)
            for d in range(1, half):
                total = total + part_in[arr, i, d, :, cols].astype(F32)
            if arr == 0:
                cdf = 0.5 * (1.0 + lax.erf(total * 0.7071067811865476))
                density = jnp.exp(-0.5 * total * total) * 0.3989422804014327
                slope[i, :, cols] = cdf + total * density
                hid[arr, i, core, :, cols] = (total * cdf).astype(BF16)
            else:
                hid[arr, i, core, :, cols] = (total * slope[i, :, cols]).astype(BF16)

        for c in range(chunks):
            for d in range(1, half):
                arrive(part_in.at[arr, i, d, :, chunk(c)], b_sem, (arr, i, d, c))
            tiles(hidden // chunks, body, c * (hidden // chunks))
            mine = hid.at[arr, i, core, :, chunk(c)]
            send(mine, mine, c_sem, (arr, i, c), {"gz": partner})

    def expand(arr, i):
        for c in range(chunks):
            arrive(hid.at[arr, i, 1 - core, :, chunk(c)], c_sem, (arr, i, c))
        left = hid.at[arr, i]

        def body(cols):
            lhs = left[...].reshape(rows, hidden)
            if arr == 0:
                out = contract(lhs, wout[:, cols], ((1,), (0,)))
            else:
                out = contract(lhs, win[cols, :], ((1,), (1,)))
            mine_sum[arr, i, :, cols] = out[:t]
            for e in range(1, nx):
                cross[arr, i, e - 1, :, cols] = out[e * t:(e + 1) * t].astype(BF16)

        by_line = via(REDUCE_VIA, arr, i)
        for p in range(PIECES):
            tiles(width // PIECES, body, p * (width // PIECES))
            if i == 0 and REDUCE_VIA[arr]:
                continue
            for e in range(1, nx):
                src = cross.at[arr, i, e - 1, :, piece(p)]
                turn = 1 - heading[i]
                send(
                    src, v_in.at[arr, turn, e - 1, :, piece(p)], d_v, (arr, turn, e, p),
                    {"gy": y - step_of[i]}, by_line,
                )
                send(
                    src, y_in.at[arr, i, nx - e - 1, :, piece(p)], d_y, (arr, i, nx - e, p),
                    peer(e), negate(by_line),
                )

    def own_cross(arr):
        if not REDUCE_VIA[arr]:
            return
        for p in range(PIECES):
            for e in range(1, nx):
                for turn, pred in ((0, has_down), (1, has_up)):
                    def take(turn=turn):
                        got = v_in.at[arr, turn, e - 1, :, piece(p)]
                        arrive(got, d_v, (arr, turn, e, p))

                        def body(cols):
                            total = cross[arr, 0, e - 1, :, cols].astype(F32)
                            total = total + v_in[arr, turn, e - 1, :, cols].astype(F32)
                            cross[arr, 0, e - 1, :, cols] = total.astype(BF16)

                        tiles(width // PIECES, body, p * (width // PIECES))

                    when(pred, take)
                src = cross.at[arr, 0, e - 1, :, piece(p)]
                send(
                    src, y_in.at[arr, 0, nx - e - 1, :, piece(p)], d_y, (arr, 0, nx - e, p),
                    peer(e),
                )

    def reduce(arr, i):
        by_line = via(REDUCE_VIA, arr, i)

        def from_columns(p):
            for e in range(1, nx):
                arrive(y_in.at[arr, i, e - 1, :, piece(p)], d_y, (arr, i, e, p))

            def body(cols):
                total = mine_sum[arr, i, :, cols]
                for e in range(1, nx):
                    total = total + y_in[arr, i, e - 1, :, cols].astype(F32)
                mine_sum[arr, i, :, cols] = total

            tiles(width // PIECES, body, p * (width // PIECES))

        def from_line(p, turn, at):
            arrive(z_in.at[arr, turn, at, :, piece(p)], d_z, (arr, turn, at, p))

            def body(cols):
                total = mine_sum[arr, i, :, cols] + z_in[arr, turn, at, :, cols].astype(F32)
                mine_sum[arr, i, :, cols] = total

            tiles(width // PIECES, body, p * (width // PIECES))

        out = (mlp_ref, tgrad_ref)[arr]
        for p in range(PIECES):
            when(negate(by_line), lambda: from_columns(p))
            if i == 0:
                when(has_down, lambda: from_line(p, 0, y))
                when(has_up, lambda: from_line(p, 1, y))
                out[:, piece(p)] = mine_sum[arr, 0, :, piece(p)].astype(BF16)
                continue
            turn = 1 - heading[i]
            when(beyond[i], lambda: from_line(p, turn, near[i]))

            def body(cols):
                fold[arr, i, :, cols] = mine_sum[arr, i, :, cols].astype(BF16)

            tiles(width // PIECES, body, p * (width // PIECES))
            send(
                fold.at[arr, i, :, piece(p)], z_in.at[arr, turn, near[i], :, piece(p)],
                d_z, (arr, turn, near[i], p), {"gy": y - step_of[i]},
            )

    def store(arr):
        for src, dst, at in (
            (rows_all.at[arr], (tok_out, grad_out)[arr], 4 + arr),
        ):
            stores.append(pltpu.make_async_copy(src, dst, local.at[at]))
            stores[-1].start()
        for i in range(ny):
            out = (act_out, dpre_out)[arr].at[near[i]]
            stores.append(pltpu.make_async_copy(hid.at[arr, i], out, local.at[6 + arr * ny + i]))
            stores[-1].start()

    acts = {
        "Fo": own_column, "Fc": other_columns, "P": project, "J": join, "G": activate,
        "E": expand, "R": reduce,
        "Fy": lambda arr, i: own_columns(arr), "Fz": lambda arr, i: own_line(arr),
        "X": lambda arr, i: own_cross(arr), "S": lambda arr, i: store(arr),
    }
    for name, arr, i in (schedule(ny) if ny == 4 else simple_schedule(ny)):
        acts[name](arr, i)
    for pred, copy in sends:
        when(pred, copy.wait_send)
    for copy in stores:
        copy.wait()


def grad_kernel(scale, tok_ref, dpre_ref, act_ref, grad_ref, win_ref, wout_ref):
    win_ref[...] = contract(tok_ref[...], dpre_ref[...], ((0,), (0,))) * scale
    wout_ref[...] = contract(act_ref[...], grad_ref[...], ((0,), (0,))) * scale


def weight_grads(tok, dpre, act, grad, scale):
    tokens, width = tok.shape
    hidden = dpre.shape[1]
    steps = next(n for n in (6, 3, 2, 1) if width % (128 * n) == 0 and hidden % (128 * n) == 0)
    wide, tall = width // steps, hidden // steps
    return pl.pallas_call(
        functools.partial(grad_kernel, scale),
        grid=(steps,),
        out_shape=(
            jax.ShapeDtypeStruct((width, hidden), F32), jax.ShapeDtypeStruct((hidden, width), F32),
        ),
        in_specs=[
            pl.BlockSpec((tokens, wide), lambda i: (0, i)),
            pl.BlockSpec((tokens, hidden), lambda i: (0, 0)),
            pl.BlockSpec((tokens, tall), lambda i: (0, i)),
            pl.BlockSpec((tokens, width), lambda i: (0, 0)),
        ],
        out_specs=(
            pl.BlockSpec((wide, hidden), lambda i: (i, 0)),
            pl.BlockSpec((tall, width), lambda i: (i, 0)),
        ),
        compiler_params=pltpu.CompilerParams(vmem_limit_bytes=48 * 2**20),
        cost_estimate=pl.CostEstimate(
            flops=4 * tokens * width * hidden, transcendentals=0,
            bytes_accessed=8 * width * hidden + 4 * tokens * (width + hidden),
        ),
    )(tok, dpre, act, grad)


def per_device(nx, ny, nz, tokens, grad_out, w_in, w_out):
    t, width = tokens.shape
    hidden = w_in.shape[1]
    rows = nx * t
    share = rows // 2
    half = nz // 2
    scale = 1.0 / math.sqrt(ny * t)
    anywhere = pl.BlockSpec(memory_space=pl.ANY)
    vmem = pl.BlockSpec(memory_space=pltpu.VMEM)
    dma = lambda *shape: pltpu.SemaphoreType.DMA((2, *shape))
    shape = jax.ShapeDtypeStruct
    mlp_out, tok_grad, tok_all, grad_all, act_all, d_pre_all = pl.pallas_call(
        functools.partial(ring_kernel, nx, ny, nz),
        out_shape=(
            shape((t, width), BF16), shape((t, width), BF16),
            shape((ny, nx, t, width), BF16), shape((ny, nx, t, width), BF16),
            shape((ny, 2, share, hidden), BF16), shape((ny, 2, share, hidden), BF16),
        ),
        in_specs=[anywhere] * 4,
        out_specs=(vmem, vmem, anywhere, anywhere, anywhere, anywhere),
        scratch_shapes=[
            pltpu.VMEM((2, ny, nx, t, width), BF16),
            pltpu.VMEM(w_in.shape, BF16),
            pltpu.VMEM(w_out.shape, BF16),
            pltpu.VMEM((2, ny, 2, share, hidden), BF16),
            pltpu.VMEM((2, ny, share, hidden), BF16),
            pltpu.VMEM((2, ny, share, hidden), BF16),
            pltpu.VMEM((2, ny, half, share, hidden), BF16),
            pltpu.VMEM((ny, share, hidden), F32),
            pltpu.VMEM((2, ny, 2, share, hidden), BF16),
            pltpu.VMEM((2, ny, t, width), F32),
            pltpu.VMEM((2, ny, nx - 1, t, width), BF16),
            pltpu.VMEM((2, ny, nx - 1, t, width), BF16),
            pltpu.VMEM((2, 2, ny, t, width), BF16),
            pltpu.VMEM((2, 2, nx - 1, t, width), BF16),
            pltpu.VMEM((2, ny, t, width), BF16),
            pltpu.SemaphoreType.DMA((6 + 2 * ny,)),
            dma(2, ny, nx, PIECES), dma(2, 2, ny, PIECES), dma(2, 2, nx, PIECES),
            dma(2, ny, CHUNKS), dma(2, ny, half, CHUNKS), dma(2, ny, CHUNKS),
            dma(2, ny, nx, PIECES), dma(2, 2, ny, PIECES), dma(2, 2, nx, PIECES),
        ],
        compiler_params=pltpu.CompilerParams(
            collective_id=0, has_side_effects=True, vmem_limit_bytes=60 * 2**20
        ),
    )(tokens, grad_out, w_in, w_out)
    tok_all, grad_all = tok_all.reshape(-1, width), grad_all.reshape(-1, width)
    act_all, d_pre_all = act_all.reshape(-1, hidden), d_pre_all.reshape(-1, hidden)
    win_grad, wout_grad = weight_grads(tok_all, d_pre_all, act_all, grad_all, scale)
    return mlp_out, tok_grad, win_grad, wout_grad


def solution(mesh):
    rows_spec = P(("gx", "gy"), "gz")
    in_spec = P("gz", ("gy", "gx"))
    out_spec = P(("gy", "gx"), "gz")
    sizes = (mesh.shape["gx"], mesh.shape["gy"], mesh.shape["gz"])
    return jax.shard_map(
        functools.partial(per_device, *sizes),
        mesh=mesh,
        in_specs=(rows_spec, rows_spec, in_spec, out_spec),
        out_specs=(rows_spec, rows_spec, in_spec, out_spec),
        check_vma=False,
    )
```

```python
import functools
import math

import jax
import jax.numpy as jnp
from jax import lax
from jax.experimental import pallas as pl
from jax.experimental.pallas import tpu as pltpu
from jax.sharding import PartitionSpec as P

MESH = pl.DeviceIdType.MESH
F32, BF16 = jnp.float32, jnp.bfloat16

GATHER_VIA = (False, False)
REDUCE_VIA = (True, False)
PIECES = 2
CHUNKS = 2
WIDE = 768
FLUSHES = 2
PLAN = (
    "Y000", "Z000", "Y001", "Z001", "W100", "Y100", "F010", "W000", "Z100", "T100", "C000",
    "C001", "F020", "F011", "P000", "P001", "F021", "T101", "F030", "C020", "J000", "F031",
    "F110", "Z101", "J001", "C010", "C100", "C011", "P010", "T000", "J010", "C021", "F120",
    "P020", "G000", "P011", "C030", "F111", "J020", "P021", "J011", "F121", "C031", "P030",
    "G010", "P031", "J030", "F130", "C110", "J031", "G001", "J021", "G020", "F131", "C111",
    "G011", "Y101", "P110", "C120", "C121", "P120", "P121", "G030", "E010", "G031", "J110",
    "E011", "P111", "C130", "E030", "C131", "G021", "P130", "P131", "E031", "C101", "J130",
    "E020", "E000", "J131", "J120", "E021", "G110", "R030", "T001", "R031", "X000", "G130",
    "G131", "J121", "P100", "E130", "R020", "J111", "P101", "G120", "E131", "R010", "R021",
    "J100", "G121", "E120", "G111", "E121", "E110", "R130", "J101", "E111", "R000", "G100",
    "R131", "E001", "R120", "X001", "G101", "R110", "E100", "R121", "R011", "E101", "R111",
    "R001", "R100", "R101",
)


def contract(left, right, dims):
    return lax.dot_general(left, right, (dims, ((), ())), preferred_element_type=F32)


def order_table(ny):
    centre = (ny - 1) / 2
    return [
        sorted(range(ny), key=lambda k: (abs(k - z), abs(k - centre))) for z in range(ny)
    ]


def schedule(ny):
    steps = [("W", 0, 0), ("W", 1, 0), ("T", 0, 0), ("T", 1, 0)]
    for arr in range(2):
        steps += [("Y", arr, 0), ("Z", arr, 0)]
        steps += [("F", arr, i) for i in range(1, ny)] + [("C", arr, i) for i in range(ny)]
        for name in "PJGE":
            steps += [(name, arr, i) for i in range(ny)]
        steps += [("X", arr, 0)]
    for arr in range(2):
        steps += [("R", arr, i) for i in reversed(range(ny))]
    steps = [(*step, p) for step in steps for p in range(PIECES) if step[0] != "W" or p == 0]
    if ny == 4:
        steps = [(step[0], *map(int, step[1:])) for step in PLAN]
    for arr in range(2):
        last = max(at for at, step in enumerate(steps) if step[:2] == ("E", arr))
        steps.insert(last + 1, ("S", arr, 0, 0))
    return steps


def ring_kernel(
    nx, ny, nz,
    tok_ref, grad_ref, win_ref, wout_ref,
    mlp_ref, tgrad_ref, tok_out, grad_out, act_out, dpre_out,
    rows_all, win, wout, win_t, wout_t, part, pair_in, paired, part_in, slope, hid,
    mine_sum, cross, y_in, z_in, v_in, fold,
    local, a_y, a_z, a_v, p_sem, b_sem, c_sem, d_y, d_z, d_v,
):
    x, y, z = lax.axis_index("gx"), lax.axis_index("gy"), lax.axis_index("gz")
    t, width = tok_ref.shape
    hidden = win_ref.shape[1]
    rows = nx * t
    share = rows // 2
    half = nz // 2
    chunks = CHUNKS if hidden % (128 * CHUNKS) == 0 else 1
    core, chip = lax.rem(z, 2), lax.div(z, 2)
    partner = z + 1 - 2 * core
    sends = []

    def pick(values):
        total = 0
        for at, value in enumerate(values):
            total = total + jnp.where(y == at, value, 0)
        return total

    table = order_table(ny)
    near = [pick([table[at][i] for at in range(ny)]) for i in range(ny)]
    gap = [pick([abs(table[at][i] - at) for at in range(ny)]) for i in range(ny)]
    gaps = [{abs(table[at][i] - at) for at in range(ny)} for i in range(ny)]
    heading = [jnp.where(near[i] < y, 0, 1) for i in range(ny)]
    step_of = [1 - 2 * heading[i] for i in range(ny)]
    beyond = [
        jnp.logical_or(
            jnp.logical_and(near[i] < y, y < ny - 1), jnp.logical_and(near[i] > y, y > 0)
        )
        for i in range(ny)
    ]
    has_up, has_down = y < ny - 1, y > 0

    def via(flags, arr, i):
        if not flags[arr] or i == 0 or 1 not in gaps[i]:
            return False
        if gaps[i] == {1}:
            return True
        return gap[i] == 1

    def when(pred, body):
        if pred is True:
            body()
        elif pred is not False:
            pl.when(pred)(body)

    def negate(pred):
        return (not pred) if isinstance(pred, bool) else jnp.logical_not(pred)

    def remote(src, dst, sems, index, device):
        return pltpu.make_async_remote_copy(
            src_ref=src, dst_ref=dst, send_sem=sems.at[(0, *index)],
            recv_sem=sems.at[(1, *index)], device_id=device, device_id_type=MESH,
        )

    def send(src, dst, sems, index, device, pred=True):
        if pred is False:
            return
        copy = remote(src, dst, sems, index, device)
        when(pred, copy.start)
        sends.append((pred, copy))

    def arrive(ref, sems, index):
        remote(ref, ref, sems, index, {"gz": z}).wait_recv()

    def peer(e):
        return {"gx": lax.rem(x + e, nx)}

    def piece(p):
        return pl.ds(p * (width // PIECES), width // PIECES)

    def chunk(c):
        return pl.ds(c * (hidden // chunks), hidden // chunks)

    def tiles(size, body, base=0, widest=256):
        tile = next(n for n in (widest, 256, 128) if size % n == 0)

        def step(i, carry):
            body(pl.ds(pl.multiple_of(base + i * tile, 128), tile))
            return carry

        lax.fori_loop(0, size // tile, step, 0)

    stage = [
        pltpu.make_async_copy(tok_ref, rows_all.at[0, y, 0], local.at[0]),
        pltpu.make_async_copy(grad_ref, rows_all.at[1, y, 0], local.at[1]),
        pltpu.make_async_copy(win_ref, win, local.at[2]),
        pltpu.make_async_copy(wout_ref, wout, local.at[3]),
    ]
    for copy in stage:
        copy.start()
    barrier = pltpu.get_barrier_semaphore()
    for name, me, n in (("gx", x, nx), ("gy", y, ny), ("gz", z, nz)):
        for d in range(1, n):
            pl.semaphore_signal(
                barrier, inc=1, device_id={name: lax.rem(me + d, n)}, device_id_type=MESH
            )
    pl.semaphore_wait(barrier, nx + ny + nz - 3)
    stores = []

    def to_columns(arr, i, p, pred=True):
        block = rows_all.at[arr, near[i], 0, :, piece(p)]
        for e in range(1, nx):
            dst = rows_all.at[arr, near[i], nx - e, :, piece(p)]
            send(block, dst, a_y, (arr, i, nx - e - 1, p), peer(e), pred)

    def own_columns(arr, i, p):
        if p == 0:
            stage[arr].wait()
        to_columns(arr, 0, p)

    def own_line(arr, i, p):
        block = rows_all.at[arr, y, 0, :, piece(p)]
        send(block, block, a_z, (arr, 0, y, p), {"gy": y + 1}, has_up)
        send(block, block, a_z, (arr, 1, y, p), {"gy": y - 1}, has_down)

    def own_column(arr, i, p):
        block = rows_all.at[arr, near[i], 0, :, piece(p)]
        arrive(block, a_z, (arr, heading[i], near[i], p))
        send(
            block, block, a_z, (arr, heading[i], near[i], p),
            {"gy": y + step_of[i]}, beyond[i],
        )
        to_columns(arr, i, p, negate(via(GATHER_VIA, arr, i)))

    def other_columns(arr, i, p):
        by_line = via(GATHER_VIA, arr, i)
        for e in range(1, nx):
            block = rows_all.at[arr, near[i], e, :, piece(p)]
            when(by_line, lambda: arrive(block, a_v, (arr, heading[i], e - 1, p)))
            when(negate(by_line), lambda: arrive(block, a_y, (arr, i, e - 1, p)))
            if i == 0 and GATHER_VIA[arr]:
                send(block, block, a_v, (arr, 0, e - 1, p), {"gy": y + 1}, has_up)
                send(block, block, a_v, (arr, 1, e - 1, p), {"gy": y - 1}, has_down)

    def turn_over(arr, i, p):
        src, dst = ((win, win_t), (wout, wout_t))[arr]
        side = src.shape[0] // PIECES
        tall = 256 if side % 256 == 0 else 128
        for j in range(side // tall):
            at = p * side + j * tall
            def body(cols):
                dst[cols, at:at + tall] = src[at:at + tall, cols].T
            tiles(src.shape[1], body)

    def project(arr, i, c):
        left = rows_all.at[arr, near[i]]

        def body(cols):
            lhs = left[...].reshape(rows, width)
            out = contract(lhs, (win, wout_t)[arr][:, cols], ((1,), (0,)))
            part[arr, i, :, :, cols] = out.astype(BF16).reshape(2, share, -1)

        tiles(hidden // chunks, body, c * (hidden // chunks), WIDE)
        send(
            part.at[arr, i, 1 - core, :, chunk(c)], pair_in.at[arr, i, :, chunk(c)],
            p_sem, (arr, i, c), {"gz": partner},
        )

    def join(arr, i, c):
        def body(cols):
            total = part[arr, i, core, :, cols].astype(F32)
            total = total + pair_in[arr, i, :, cols].astype(F32)
            paired[arr, i, :, cols] = total.astype(BF16)

        arrive(pair_in.at[arr, i, :, chunk(c)], p_sem, (arr, i, c))
        tiles(hidden // chunks, body, c * (hidden // chunks))
        for d in range(1, half):
            to = lax.rem(chip + d, half)
            send(
                paired.at[arr, i, :, chunk(c)], part_in.at[arr, i, d - 1, :, chunk(c)],
                b_sem, (arr, i, d - 1, c), {"gz": 2 * to + core},
            )

    def activate(arr, i, c):
        def body(cols):
            total = paired[arr, i, :, cols].astype(F32)
            for d in range(1, half):
                total = total + part_in[arr, i, d - 1, :, cols].astype(F32)
            if arr == 0:
                cdf = 0.5 * (1.0 + lax.erf(total * 0.7071067811865476))
                density = jnp.exp(-0.5 * total * total) * 0.3989422804014327
                slope[i, :, cols] = cdf + total * density
                hid[arr, i, core, :, cols] = (total * cdf).astype(BF16)
            else:
                hid[arr, i, core, :, cols] = (total * slope[i, :, cols]).astype(BF16)

        for d in range(1, half):
            arrive(part_in.at[arr, i, d - 1, :, chunk(c)], b_sem, (arr, i, d - 1, c))
        tiles(hidden // chunks, body, c * (hidden // chunks))
        mine = hid.at[arr, i, core, :, chunk(c)]
        send(mine, mine, c_sem, (arr, i, c), {"gz": partner})

    def expand(arr, i, p):
        if p == 0:
            for c in range(chunks):
                arrive(hid.at[arr, i, 1 - core, :, chunk(c)], c_sem, (arr, i, c))
        left = hid.at[arr, i]

        def body(cols):
            lhs = left[...].reshape(rows, hidden)
            out = contract(lhs, (wout, win_t)[arr][:, cols], ((1,), (0,)))
            mine_sum[arr, i, :, cols] = out[:t]
            for e in range(1, nx):
                cross[arr, i, e - 1, :, cols] = out[e * t:(e + 1) * t].astype(BF16)

        by_line = via(REDUCE_VIA, arr, i)
        tiles(width // PIECES, body, p * (width // PIECES), WIDE)
        if i == 0 and REDUCE_VIA[arr]:
            return
        for e in range(1, nx):
            src = cross.at[arr, i, e - 1, :, piece(p)]
            turn = 1 - heading[i]
            send(
                src, v_in.at[arr, turn, e - 1, :, piece(p)], d_v, (arr, turn, e - 1, p),
                {"gy": y - step_of[i]}, by_line,
            )
            send(
                src, y_in.at[arr, i, nx - e - 1, :, piece(p)], d_y, (arr, i, nx - e - 1, p),
                peer(e), negate(by_line),
            )

    def own_cross(arr, i, p):
        if not REDUCE_VIA[arr]:
            return
        for e in range(1, nx):
            for turn, pred in ((0, has_down), (1, has_up)):
                def take(turn=turn):
                    got = v_in.at[arr, turn, e - 1, :, piece(p)]
                    arrive(got, d_v, (arr, turn, e - 1, p))

                    def body(cols):
                        total = cross[arr, 0, e - 1, :, cols].astype(F32)
                        total = total + v_in[arr, turn, e - 1, :, cols].astype(F32)
                        cross[arr, 0, e - 1, :, cols] = total.astype(BF16)

                    tiles(width // PIECES, body, p * (width // PIECES))

                when(pred, take)
            src = cross.at[arr, 0, e - 1, :, piece(p)]
            send(
                src, y_in.at[arr, 0, nx - e - 1, :, piece(p)], d_y, (arr, 0, nx - e - 1, p),
                peer(e),
            )

    def reduce(arr, i, p):
        by_line = via(REDUCE_VIA, arr, i)

        def from_columns():
            for e in range(1, nx):
                arrive(y_in.at[arr, i, e - 1, :, piece(p)], d_y, (arr, i, e - 1, p))

            def body(cols):
                total = mine_sum[arr, i, :, cols]
                for e in range(1, nx):
                    total = total + y_in[arr, i, e - 1, :, cols].astype(F32)
                mine_sum[arr, i, :, cols] = total

            tiles(width // PIECES, body, p * (width // PIECES))

        def from_line(turn, at):
            arrive(z_in.at[arr, turn, at, :, piece(p)], d_z, (arr, turn, at, p))

            def body(cols):
                total = mine_sum[arr, i, :, cols] + z_in[arr, turn, at, :, cols].astype(F32)
                mine_sum[arr, i, :, cols] = total

            tiles(width // PIECES, body, p * (width // PIECES))

        out = (mlp_ref, tgrad_ref)[arr]
        when(negate(by_line), from_columns)
        if i == 0:
            when(has_down, lambda: from_line(0, y))
            when(has_up, lambda: from_line(1, y))
            out[:, piece(p)] = mine_sum[arr, 0, :, piece(p)].astype(BF16)
            return
        turn = 1 - heading[i]
        when(beyond[i], lambda: from_line(turn, near[i]))

        def body(cols):
            fold[arr, i, :, cols] = mine_sum[arr, i, :, cols].astype(BF16)

        tiles(width // PIECES, body, p * (width // PIECES))
        send(
            fold.at[arr, i, :, piece(p)], z_in.at[arr, turn, near[i], :, piece(p)],
            d_z, (arr, turn, near[i], p), {"gy": y - step_of[i]},
        )

    def store(arr, i, p):
        stores.append(
            pltpu.make_async_copy(rows_all.at[arr], (tok_out, grad_out)[arr], local.at[4 + arr])
        )
        stores[-1].start()
        for i in range(ny):
            out = (act_out, dpre_out)[arr].at[near[i]]
            stores.append(pltpu.make_async_copy(hid.at[arr, i], out, local.at[6 + arr * ny + i]))
            stores[-1].start()

    acts = {
        "Y": own_columns, "Z": own_line, "F": own_column, "C": other_columns, "T": turn_over,
        "P": project, "J": join, "G": activate, "E": expand, "X": own_cross, "R": reduce,
        "S": store, "W": lambda arr, i, p: stage[2 + arr].wait(),
    }
    def flush(count):
        for pred, copy in sends[:count]:
            when(pred, copy.wait_send)
        del sends[:count]

    steps = schedule(ny)
    marks = [at for at, step in enumerate(steps) if step[0] == "R"][-FLUSHES:]
    before = 0
    for at, (name, arr, i, p) in enumerate(steps):
        if name in "PJG" and p >= chunks:
            continue
        if at in marks:
            flush(before)
        before = len(sends)
        acts[name](arr, i, p)
    flush(len(sends))
    for copy in stores:
        copy.wait()


def grad_kernel(scale, tok_ref, dpre_ref, act_ref, grad_ref, win_ref, wout_ref):
    win_ref[...] = contract(tok_ref[...], dpre_ref[...], ((0,), (0,))) * scale
    wout_ref[...] = contract(act_ref[...], grad_ref[...], ((0,), (0,))) * scale


def weight_grads(tok, dpre, act, grad, scale):
    tokens, width = tok.shape
    hidden = dpre.shape[1]
    steps = next(n for n in (6, 3, 2, 1) if width % (128 * n) == 0 and hidden % (128 * n) == 0)
    wide, tall = width // steps, hidden // steps
    return pl.pallas_call(
        functools.partial(grad_kernel, scale),
        grid=(steps,),
        out_shape=(
            jax.ShapeDtypeStruct((width, hidden), F32), jax.ShapeDtypeStruct((hidden, width), F32),
        ),
        in_specs=[
            pl.BlockSpec((tokens, wide), lambda i: (0, i)),
            pl.BlockSpec((tokens, hidden), lambda i: (0, 0)),
            pl.BlockSpec((tokens, tall), lambda i: (0, i)),
            pl.BlockSpec((tokens, width), lambda i: (0, 0)),
        ],
        out_specs=(
            pl.BlockSpec((wide, hidden), lambda i: (i, 0)),
            pl.BlockSpec((tall, width), lambda i: (i, 0)),
        ),
        compiler_params=pltpu.CompilerParams(vmem_limit_bytes=60 * 2**20),
        cost_estimate=pl.CostEstimate(
            flops=4 * tokens * width * hidden, transcendentals=0,
            bytes_accessed=8 * width * hidden + 4 * tokens * (width + hidden),
        ),
    )(tok, dpre, act, grad)


def per_device(nx, ny, nz, tokens, grad_out, w_in, w_out):
    t, width = tokens.shape
    hidden = w_in.shape[1]
    rows = nx * t
    share = rows // 2
    half = nz // 2
    scale = 1.0 / math.sqrt(ny * t)
    anywhere = pl.BlockSpec(memory_space=pl.ANY)
    vmem = pl.BlockSpec(memory_space=pltpu.VMEM)
    dma = lambda *shape: pltpu.SemaphoreType.DMA((2, *shape))
    shape = jax.ShapeDtypeStruct
    mlp_out, tok_grad, tok_all, grad_all, act_all, d_pre_all = pl.pallas_call(
        functools.partial(ring_kernel, nx, ny, nz),
        out_shape=(
            shape((t, width), BF16), shape((t, width), BF16),
            shape((ny, nx, t, width), BF16), shape((ny, nx, t, width), BF16),
            shape((ny, 2, share, hidden), BF16), shape((ny, 2, share, hidden), BF16),
        ),
        in_specs=[anywhere] * 4,
        out_specs=(vmem, vmem, anywhere, anywhere, anywhere, anywhere),
        scratch_shapes=[
            pltpu.VMEM((2, ny, nx, t, width), BF16),
            pltpu.VMEM(w_in.shape, BF16),
            pltpu.VMEM(w_out.shape, BF16),
            pltpu.VMEM(w_in.shape[::-1], BF16),
            pltpu.VMEM(w_out.shape[::-1], BF16),
            pltpu.VMEM((2, ny, 2, share, hidden), BF16),
            pltpu.VMEM((2, ny, share, hidden), BF16),
            pltpu.VMEM((2, ny, share, hidden), BF16),
            pltpu.VMEM((2, ny, half - 1, share, hidden), BF16),
            pltpu.VMEM((ny, share, hidden), F32),
            pltpu.VMEM((2, ny, 2, share, hidden), BF16),
            pltpu.VMEM((2, ny, t, width), F32),
            pltpu.VMEM((2, ny, nx - 1, t, width), BF16),
            pltpu.VMEM((2, ny, nx - 1, t, width), BF16),
            pltpu.VMEM((2, 2, ny, t, width), BF16),
            pltpu.VMEM((2, 2, nx - 1, t, width), BF16),
            pltpu.VMEM((2, ny, t, width), BF16),
            pltpu.SemaphoreType.DMA((6 + 2 * ny,)),
            dma(2, ny, nx - 1, PIECES), dma(2, 2, ny, PIECES), dma(2, 2, nx - 1, PIECES),
            dma(2, ny, CHUNKS), dma(2, ny, half - 1, CHUNKS), dma(2, ny, CHUNKS),
            dma(2, ny, nx - 1, PIECES), dma(2, 2, ny, PIECES), dma(2, 2, nx - 1, PIECES),
        ],
        compiler_params=pltpu.CompilerParams(
            collective_id=0, has_side_effects=True, vmem_limit_bytes=60 * 2**20
        ),
    )(tokens, grad_out, w_in, w_out)
    tok_all, grad_all = tok_all.reshape(-1, width), grad_all.reshape(-1, width)
    act_all, d_pre_all = act_all.reshape(-1, hidden), d_pre_all.reshape(-1, hidden)
    win_grad, wout_grad = weight_grads(tok_all, d_pre_all, act_all, grad_all, scale)
    return mlp_out, tok_grad, win_grad, wout_grad


def solution(mesh):
    rows_spec = P(("gx", "gy"), "gz")
    in_spec = P("gz", ("gy", "gx"))
    out_spec = P(("gy", "gx"), "gz")
    sizes = (mesh.shape["gx"], mesh.shape["gy"], mesh.shape["gz"])
    return jax.shard_map(
        functools.partial(per_device, *sizes),
        mesh=mesh,
        in_specs=(rows_spec, rows_spec, in_spec, out_spec),
        out_specs=(rows_spec, rows_spec, in_spec, out_spec),
        check_vma=False,
    )
```

```python
import functools
import math

import jax
import jax.numpy as jnp
from jax import lax
from jax.experimental import pallas as pl
from jax.experimental.pallas import tpu as pltpu
from jax.sharding import PartitionSpec as P

MESH = pl.DeviceIdType.MESH
F32, BF16 = jnp.float32, jnp.bfloat16

GATHER_VIA = (False, True)
REDUCE_VIA = (True, False)
PIECES = 2
CHUNKS = 2
WIDE = 768
KINDS = "YZFCWTPJGEXR"
PLANS = (
    (
        1000, 1001, 2000, 2001, 3010, 1100, 2100, 5000, 2101, 4000, 4001, 3011, 4010, 3020,
        4100, 3021, 5100, 3030, 4011, 7010, 8010, 7000, 8000, 4020, 3031, 4021, 7020, 7011,
        7021, 1101, 8020, 8011, 9010, 4030, 3110, 3130, 4031, 8021, 3131, 6100, 7030, 7001,
        7031, 4101, 9020, 8030, 9011, 3120, 6101, 9000, 8031, 8001, 3111, 4130, 9021, 3121,
        4131, 10010, 7130, 10020, 7100, 7131, 12010, 9030, 10021, 8100, 10011, 4120, 9031, 8130,
        4121, 7120, 7101, 4110, 4111, 8131, 10030, 9001, 7110, 10031, 12020, 10000, 11000, 7111,
        10001, 7121, 8120, 12011, 6000, 8121, 8110, 11001, 9130, 9100, 9131, 12030, 6001, 12031,
        10130, 8111, 9120, 12021, 10131, 8101, 9121, 10120, 12130, 10121, 9110, 9111, 12131, 10110,
        12120, 9101, 10111, 10100, 12121, 10101, 12110, 12000, 12111, 12001, 12100, 12101,
    ),
    (
        1000, 1001, 2000, 2001, 3020, 3010, 3011, 3021, 4000, 5000, 3120, 3030, 3121, 4010,
        3031, 3130, 4011, 4001, 5100, 7010, 7000, 8010, 4020, 1100, 4021, 2100, 7020, 3131,
        2101, 8020, 4030, 1101, 7011, 8000, 7021, 9010, 3110, 8011, 4031, 6100, 7030, 7001,
        7031, 9020, 8021, 8030, 3111, 9000, 8031, 4130, 4120, 9011, 4100, 6101, 9021, 4131,
        8001, 4101, 10010, 7130, 10020, 7100, 4110, 7131, 10021, 10011, 9030, 9031, 4121, 8130,
        4111, 7120, 7101, 10030, 9001, 8131, 7110, 10031, 10000, 11000, 8120, 7111, 10001, 7121,
        8110, 6000, 12010, 8121, 9130, 11001, 9131, 6001, 9120, 10130, 8100, 10131, 8111, 12030,
        9110, 8101, 9121, 10120, 12031, 10121, 12011, 9111, 12020, 12000, 9100, 10110, 12130, 9101,
        10111, 10100, 12131, 12021, 10101, 12110, 12120, 12001, 12111, 12121, 12100, 12101,
    ),
)


def contract(left, right, dims):
    return lax.dot_general(left, right, (dims, ((), ())), preferred_element_type=F32)


def order_table(ny):
    centre = (ny - 1) / 2
    return [
        sorted(range(ny), key=lambda k: (abs(k - z), abs(k - centre))) for z in range(ny)
    ]


def schedule(ny):
    steps = [("W", 0, 0), ("W", 1, 0), ("T", 0, 0), ("T", 1, 0)]
    for arr in range(2):
        steps += [("Y", arr, 0), ("Z", arr, 0)]
        steps += [("F", arr, i) for i in range(1, ny)] + [("C", arr, i) for i in range(ny)]
        for name in "PJGE":
            steps += [(name, arr, i) for i in range(ny)]
        steps += [("X", arr, 0)]
    for arr in range(2):
        steps += [("R", arr, i) for i in reversed(range(ny))]
    steps = [(*step, p) for step in steps for p in range(PIECES) if step[0] != "W" or p == 0]
    plans = (steps, steps)
    if ny == 4:
        plans = [
            [
                (KINDS[step // 1000 - 1], step // 100 % 10, step // 10 % 10, step % 10)
                for step in plan
            ]
            for plan in PLANS
        ]
    cut = []
    for plan in plans:
        parts = [[]]
        for step in plan:
            if step[0] in "PET":
                parts += [step, []]
            else:
                parts[-1].append(step)
        cut.append(parts)
    out = []
    for ends, inside in zip(*cut):
        if ends == inside:
            out.append(([], [], [ends] if isinstance(ends, tuple) else ends))
        else:
            out.append((ends, inside, []))
    for arr in range(2):
        last = max(at for at, part in enumerate(out) if part[2] and part[2][0][:2] == ("E", arr))
        out.insert(last + 1, ([], [], [("S", arr, 0, 0)]))
    return out


def ring_kernel(
    nx, ny, nz,
    tok_ref, grad_ref, win_ref, wout_ref,
    mlp_ref, tgrad_ref, tok_out, grad_out, act_out, dpre_out,
    rows_all, win, wout, win_t, wout_t, part, pair_in, paired, part_in, slope, hid,
    mine_sum, cross, y_in, z_in, v_in, fold,
    local, *pairs,
):
    a_y, a_z, a_v, p_sem, b_sem, c_sem, d_y, d_z, d_v = zip(pairs[::2], pairs[1::2])
    x, y, z = lax.axis_index("gx"), lax.axis_index("gy"), lax.axis_index("gz")
    t, width = tok_ref.shape
    hidden = win_ref.shape[1]
    rows = nx * t
    share = rows // 2
    half = nz // 2
    chunks = CHUNKS if hidden % (128 * CHUNKS) == 0 else 1
    core, chip = lax.rem(z, 2), lax.div(z, 2)
    partner = z + 1 - 2 * core
    sends = {}

    def pick(values):
        total = 0
        for at, value in enumerate(values):
            total = total + jnp.where(y == at, value, 0)
        return total

    table = order_table(ny)
    near = [pick([table[at][i] for at in range(ny)]) for i in range(ny)]
    gap = [pick([abs(table[at][i] - at) for at in range(ny)]) for i in range(ny)]
    gaps = [{abs(table[at][i] - at) for at in range(ny)} for i in range(ny)]
    heading = [jnp.where(near[i] < y, 0, 1) for i in range(ny)]
    step_of = [1 - 2 * heading[i] for i in range(ny)]
    back = [1 - heading[i] for i in range(ny)]
    beyond = [
        jnp.logical_or(
            jnp.logical_and(near[i] < y, y < ny - 1), jnp.logical_and(near[i] > y, y > 0)
        )
        for i in range(ny)
    ]
    has_up, has_down = y < ny - 1, y > 0
    at_end = jnp.logical_or(y == 0, y == ny - 1)
    inside = jnp.logical_not(at_end)
    role = [None]

    def negate(pred):
        return (not pred) if isinstance(pred, bool) else jnp.logical_not(pred)

    def by_line_anywhere(flags, arr, i):
        if not flags[arr] or i == 0 or 1 not in gaps[i]:
            return False
        return True if gaps[i] == {1} else gap[i] == 1

    lines = {}
    for flags in (GATHER_VIA, REDUCE_VIA):
        for arr in range(2):
            for i in range(ny):
                found = by_line_anywhere(flags, arr, i)
                lines[flags, arr, i] = (found, negate(found))

    def via(flags, arr, i):
        if role[0] is None:
            return lines[flags, arr, i]
        here = abs(order_table(ny)[1 if role[0] == "inside" else 0][i] - (role[0] == "inside"))
        return (flags[arr] and here == 1), not (flags[arr] and here == 1)

    def onward(i):
        return {None: beyond[i], "end": False, "inside": True}[role[0]]

    def upward():
        return True if role[0] == "inside" else has_up

    def downward():
        return True if role[0] == "inside" else has_down

    def when(pred, body):
        if pred is True:
            body()
        elif pred is not False:
            pl.when(pred)(body)

    def remote(src, dst, leaving, landing, device):
        return pltpu.make_async_remote_copy(
            src_ref=src, dst_ref=dst, send_sem=leaving, recv_sem=landing,
            device_id=device, device_id_type=MESH,
        )

    def send(src, dst, sems, index, device, pred=lambda: True, leaving=None, bulk=None, key=None):
        now = pred()
        if now is False:
            return
        leaving = index[:-1] if leaving is None else leaving
        copy = remote(src, dst, sems[0].at[leaving], sems[1].at[index], device)
        when(now, copy.start)
        sends.setdefault(key, (sems, leaving, index, bulk, pred))

    def arrive(ref, sems, index):
        leaving = sems[0].at[(0,) * len(sems[0].shape)]
        remote(ref, ref, leaving, sems[1].at[index], {"gz": z}).wait_recv()

    def depart():
        for sems, leaving, index, bulk, pred in sends.values():
            ref = rows_all.at[0, 0, 0] if bulk is None else bulk
            copy = remote(ref, ref, sems[0].at[leaving], sems[1].at[index], {"gz": z})
            when(pred(), copy.wait_send)

    def peer(e):
        return {"gx": lax.rem(x + e, nx)}

    def piece(p):
        return pl.ds(p * (width // PIECES), width // PIECES)

    def chunk(c):
        return pl.ds(c * (hidden // chunks), hidden // chunks)

    def tiles(size, body, base=0, widest=256):
        tile = next(n for n in (widest, 256, 128) if size % n == 0)

        def step(i, carry):
            body(pl.ds(pl.multiple_of(base + i * tile, 128), tile))
            return carry

        lax.fori_loop(0, size // tile, step, 0)

    stage = [
        pltpu.make_async_copy(tok_ref, rows_all.at[0, y, 0], local.at[0]),
        pltpu.make_async_copy(grad_ref, rows_all.at[1, y, 0], local.at[1]),
        pltpu.make_async_copy(win_ref, win, local.at[2]),
        pltpu.make_async_copy(wout_ref, wout, local.at[3]),
    ]
    for copy in stage:
        copy.start()
    barrier = pltpu.get_barrier_semaphore()
    for name, me, n in (("gx", x, nx), ("gy", y, ny), ("gz", z, nz)):
        for d in range(1, n):
            pl.semaphore_signal(
                barrier, inc=1, device_id={name: lax.rem(me + d, n)}, device_id_type=MESH
            )
    pl.semaphore_wait(barrier, nx + ny + nz - 3)
    stores = []

    def to_columns(arr, i, p, pred=lambda: True):
        block = rows_all.at[arr, near[i], 0, :, piece(p)]
        for e in range(1, nx):
            dst = rows_all.at[arr, near[i], nx - e, :, piece(p)]
            send(
                block, dst, a_y, (arr, i, nx - e - 1, p), peer(e), pred, key=("a_y", arr, i, e)
            )

    def own_columns(arr, i, p):
        if p == 0:
            stage[arr].wait()
        to_columns(arr, 0, p)

    def own_line(arr, i, p):
        block = rows_all.at[arr, y, 0, :, piece(p)]
        for turn, to, pred in ((0, y + 1, upward), (1, y - 1, downward)):
            send(
                block, block, a_z, (arr, y, p), {"gy": to}, pred, (arr, turn, y),
                key=("a_z", arr, turn),
            )

    def own_column(arr, i, p):
        block = rows_all.at[arr, near[i], 0, :, piece(p)]
        arrive(block, a_z, (arr, near[i], p))
        send(
            block, block, a_z, (arr, near[i], p), {"gy": y + step_of[i]}, lambda: onward(i),
            (arr, heading[i], near[i]), key=("a_z", arr, i, 0),
        )
        to_columns(arr, i, p, lambda: via(GATHER_VIA, arr, i)[1])

    def other_columns(arr, i, p):
        by_line, by_column = via(GATHER_VIA, arr, i)
        for e in range(1, nx):
            block = rows_all.at[arr, near[i], e, :, piece(p)]
            when(by_line, lambda: arrive(block, a_v, (arr, heading[i], e - 1, p)))
            when(by_column, lambda: arrive(block, a_y, (arr, i, e - 1, p)))
            if i == 0 and GATHER_VIA[arr]:
                for turn, to, pred in ((0, y + 1, upward), (1, y - 1, downward)):
                    send(
                        block, block, a_v, (arr, turn, e - 1, p), {"gy": to}, pred,
                        key=("a_v", arr, turn, e),
                    )

    def turn_over(arr, i, p):
        src, dst = ((win, win_t), (wout, wout_t))[arr]
        side = src.shape[0] // PIECES
        tall = 256 if side % 256 == 0 else 128
        for j in range(side // tall):
            at = p * side + j * tall
            def body(cols):
                dst[cols, at:at + tall] = src[at:at + tall, cols].T
            tiles(src.shape[1], body)

    def project(arr, i, c):
        left = rows_all.at[arr, near[i]]

        def body(cols):
            lhs = left[...].reshape(rows, width)
            out = contract(lhs, (win, wout_t)[arr][:, cols], ((1,), (0,)))
            part[arr, i, :, :, cols] = out.astype(BF16).reshape(2, share, -1)

        tiles(hidden // chunks, body, c * (hidden // chunks), WIDE)
        send(
            part.at[arr, i, 1 - core, :, chunk(c)], pair_in.at[arr, i, :, chunk(c)],
            p_sem, (arr, i, c), {"gz": partner}, leaving=(0,), bulk=pair_in, key="p",
        )

    def join(arr, i, c):
        def body(cols):
            total = part[arr, i, core, :, cols].astype(F32)
            total = total + pair_in[arr, i, :, cols].astype(F32)
            paired[arr, i, :, cols] = total.astype(BF16)

        arrive(pair_in.at[arr, i, :, chunk(c)], p_sem, (arr, i, c))
        tiles(hidden // chunks, body, c * (hidden // chunks))
        for d in range(1, half):
            to = lax.rem(chip + d, half)
            send(
                paired.at[arr, i, :, chunk(c)], part_in.at[arr, i, d - 1, :, chunk(c)],
                b_sem, (arr, i, d - 1, c), {"gz": 2 * to + core}, leaving=(0,), bulk=part_in,
                key="b",
            )

    def activate(arr, i, c):
        def body(cols):
            total = paired[arr, i, :, cols].astype(F32)
            for d in range(1, half):
                total = total + part_in[arr, i, d - 1, :, cols].astype(F32)
            if arr == 0:
                cdf = 0.5 * (1.0 + lax.erf(total * 0.7071067811865476))
                density = jnp.exp(-0.5 * total * total) * 0.3989422804014327
                slope[i, :, cols] = cdf + total * density
                hid[arr, i, core, :, cols] = (total * cdf).astype(BF16)
            else:
                hid[arr, i, core, :, cols] = (total * slope[i, :, cols]).astype(BF16)

        for d in range(1, half):
            arrive(part_in.at[arr, i, d - 1, :, chunk(c)], b_sem, (arr, i, d - 1, c))
        tiles(hidden // chunks, body, c * (hidden // chunks))
        mine = hid.at[arr, i, core, :, chunk(c)]
        send(
            mine, mine, c_sem, (arr, i, c), {"gz": partner}, leaving=(0,), bulk=pair_in, key="c"
        )

    def expand(arr, i, p):
        if p == 0:
            for c in range(chunks):
                arrive(hid.at[arr, i, 1 - core, :, chunk(c)], c_sem, (arr, i, c))
        left = hid.at[arr, i]

        def body(cols):
            lhs = left[...].reshape(rows, hidden)
            out = contract(lhs, (wout, win_t)[arr][:, cols], ((1,), (0,)))
            mine_sum[arr, i, :, cols] = out[:t]
            for e in range(1, nx):
                cross[arr, i, e - 1, :, cols] = out[e * t:(e + 1) * t].astype(BF16)

        tiles(width // PIECES, body, p * (width // PIECES), WIDE)
        if i == 0 and REDUCE_VIA[arr]:
            return
        for e in range(1, nx):
            src = cross.at[arr, i, e - 1, :, piece(p)]
            send(
                src, v_in.at[arr, back[i], e - 1, :, piece(p)], d_v, (arr, back[i], e - 1, p),
                {"gy": y - step_of[i]}, lambda: via(REDUCE_VIA, arr, i)[0],
                key=("d_v", arr, i, e),
            )
            send(
                src, y_in.at[arr, i, nx - e - 1, :, piece(p)], d_y, (arr, i, nx - e - 1, p),
                peer(e), lambda: via(REDUCE_VIA, arr, i)[1], key=("d_y", arr, i, e),
            )

    def own_cross(arr, i, p):
        if not REDUCE_VIA[arr]:
            return
        for e in range(1, nx):
            for turn, pred in ((0, downward()), (1, upward())):
                def take(turn=turn):
                    got = v_in.at[arr, turn, e - 1, :, piece(p)]
                    arrive(got, d_v, (arr, turn, e - 1, p))

                    def body(cols):
                        total = cross[arr, 0, e - 1, :, cols].astype(F32)
                        total = total + v_in[arr, turn, e - 1, :, cols].astype(F32)
                        cross[arr, 0, e - 1, :, cols] = total.astype(BF16)

                    tiles(width // PIECES, body, p * (width // PIECES))

                when(pred, take)
            src = cross.at[arr, 0, e - 1, :, piece(p)]
            send(
                src, y_in.at[arr, 0, nx - e - 1, :, piece(p)], d_y, (arr, 0, nx - e - 1, p),
                peer(e), key=("d_y", arr, 0, e),
            )

    def reduce(arr, i, p):
        def from_columns():
            for e in range(1, nx):
                arrive(y_in.at[arr, i, e - 1, :, piece(p)], d_y, (arr, i, e - 1, p))

            def body(cols):
                total = mine_sum[arr, i, :, cols]
                for e in range(1, nx):
                    total = total + y_in[arr, i, e - 1, :, cols].astype(F32)
                mine_sum[arr, i, :, cols] = total

            tiles(width // PIECES, body, p * (width // PIECES))

        def from_line(turn, at):
            arrive(z_in.at[arr, turn, at, :, piece(p)], d_z, (arr, turn, at, p))

            def body(cols):
                total = mine_sum[arr, i, :, cols] + z_in[arr, turn, at, :, cols].astype(F32)
                mine_sum[arr, i, :, cols] = total

            tiles(width // PIECES, body, p * (width // PIECES))

        out = (mlp_ref, tgrad_ref)[arr]
        when(via(REDUCE_VIA, arr, i)[1], from_columns)
        if i == 0:
            when(downward(), lambda: from_line(0, y))
            when(upward(), lambda: from_line(1, y))
            out[:, piece(p)] = mine_sum[arr, 0, :, piece(p)].astype(BF16)
            return
        when(onward(i), lambda: from_line(back[i], near[i]))

        def body(cols):
            fold[arr, i, :, cols] = mine_sum[arr, i, :, cols].astype(BF16)

        tiles(width // PIECES, body, p * (width // PIECES))
        send(
            fold.at[arr, i, :, piece(p)], z_in.at[arr, back[i], near[i], :, piece(p)],
            d_z, (arr, back[i], near[i], p), {"gy": y - step_of[i]}, key=("d_z", arr, i),
        )

    def store(arr, i, p):
        stores.append(
            pltpu.make_async_copy(rows_all.at[arr], (tok_out, grad_out)[arr], local.at[4 + arr])
        )
        stores[-1].start()
        for i in range(ny):
            out = (act_out, dpre_out)[arr].at[near[i]]
            stores.append(pltpu.make_async_copy(hid.at[arr, i], out, local.at[6 + arr * ny + i]))
            stores[-1].start()

    acts = {
        "Y": own_columns, "Z": own_line, "F": own_column, "C": other_columns, "T": turn_over,
        "P": project, "J": join, "G": activate, "E": expand, "X": own_cross, "R": reduce,
        "S": store, "W": lambda arr, i, p: stage[2 + arr].wait(),
    }
    def run(steps):
        for name, arr, i, p in steps:
            if name not in "PJG" or p < chunks:
                acts[name](arr, i, p)

    def run_at(steps, place, pred):
        def body():
            role[0] = place
            run(steps)
            role[0] = None

        if steps:
            pl.when(pred)(body)

    for at_ends, insides, both in schedule(ny):
        run_at(at_ends, "end", at_end)
        run_at(insides, "inside", inside)
        run(both)
    depart()
    for copy in stores:
        copy.wait()


def grad_kernel(
    scale, tok_ref, dpre_ref, act_ref, grad_ref, mlp_ref, tgrad_ref,
    win_ref, wout_ref, mlp_out, tgrad_out,
    tok, dpre, act, grad, rows, win, wout, loads, stores,
):
    def load(src, dst, at):
        copy = pltpu.make_async_copy(src, dst, loads.at[at])
        copy.start()
        return copy

    first = [load(tok_ref, tok, 0), load(dpre_ref, dpre, 1)]
    second = [load(act_ref, act, 2), load(grad_ref, grad, 3)]
    passing = [load(mlp_ref, rows.at[0], 4), load(tgrad_ref, rows.at[1], 5)]

    def product(left, right, total, out, sem):
        tall = next(n for n in (256, 128) if total.shape[0] % n == 0)

        def step(i, carry):
            part = pl.ds(pl.multiple_of(i * tall, 128), tall)
            total[part, :] = contract(left[:, part], right[...], ((0,), (0,))) * scale
            pltpu.make_async_copy(total.at[part, :], out.at[part, :], sem).start()
            return carry

        count = total.shape[0] // tall
        lax.fori_loop(0, count, step, 0, unroll=2 if count % 2 == 0 else 1)

    for copy in first:
        copy.wait()
    product(tok, dpre, win, win_ref, stores.at[0])
    for copy in second:
        copy.wait()
    product(act, grad, wout, wout_ref, stores.at[1])
    for at, out in enumerate((mlp_out, tgrad_out)):
        passing[at].wait()
        pltpu.make_async_copy(rows.at[at], out, stores.at[2 + at]).start()
    pltpu.make_async_copy(win, win_ref, stores.at[0]).wait()
    pltpu.make_async_copy(wout, wout_ref, stores.at[1]).wait()
    for at, out in enumerate((mlp_out, tgrad_out)):
        pltpu.make_async_copy(rows.at[at], out, stores.at[2 + at]).wait()


def finish(tok, dpre, act, grad, mlp, tgrad, scale):
    tokens, width = tok.shape
    hidden = dpre.shape[1]
    shape = jax.ShapeDtypeStruct
    anywhere = pl.BlockSpec(memory_space=pl.ANY)
    return pl.pallas_call(
        functools.partial(grad_kernel, scale),
        out_shape=(
            shape((width, hidden), F32), shape((hidden, width), F32),
            shape(mlp.shape, BF16), shape(tgrad.shape, BF16),
        ),
        in_specs=[anywhere] * 6,
        out_specs=(anywhere,) * 4,
        scratch_shapes=[
            pltpu.VMEM(tok.shape, BF16), pltpu.VMEM(dpre.shape, BF16),
            pltpu.VMEM(act.shape, BF16), pltpu.VMEM(grad.shape, BF16),
            pltpu.VMEM((2, *mlp.shape), BF16),
            pltpu.VMEM((width, hidden), F32), pltpu.VMEM((hidden, width), F32),
            pltpu.SemaphoreType.DMA((6,)), pltpu.SemaphoreType.DMA((4,)),
        ],
        compiler_params=pltpu.CompilerParams(vmem_limit_bytes=60 * 2**20),
        cost_estimate=pl.CostEstimate(
            flops=4 * tokens * width * hidden, transcendentals=0,
            bytes_accessed=8 * width * hidden + 4 * tokens * (width + hidden),
        ),
    )(tok, dpre, act, grad, mlp, tgrad)


def per_device(nx, ny, nz, tokens, grad_out, w_in, w_out):
    t, width = tokens.shape
    hidden = w_in.shape[1]
    rows = nx * t
    share = rows // 2
    half = nz // 2
    scale = 1.0 / math.sqrt(ny * t)
    anywhere = pl.BlockSpec(memory_space=pl.ANY)
    vmem = pl.BlockSpec(memory_space=pltpu.VMEM)
    dma = lambda *shape: pltpu.SemaphoreType.DMA(shape)
    shape = jax.ShapeDtypeStruct
    mlp_out, tok_grad, tok_all, grad_all, act_all, d_pre_all = pl.pallas_call(
        functools.partial(ring_kernel, nx, ny, nz),
        out_shape=(
            shape((t, width), BF16), shape((t, width), BF16),
            shape((ny, nx, t, width), BF16), shape((ny, nx, t, width), BF16),
            shape((ny, 2, share, hidden), BF16), shape((ny, 2, share, hidden), BF16),
        ),
        in_specs=[anywhere] * 4,
        out_specs=(vmem, vmem, anywhere, anywhere, anywhere, anywhere),
        scratch_shapes=[
            pltpu.VMEM((2, ny, nx, t, width), BF16),
            pltpu.VMEM(w_in.shape, BF16),
            pltpu.VMEM(w_out.shape, BF16),
            pltpu.VMEM(w_in.shape[::-1], BF16),
            pltpu.VMEM(w_out.shape[::-1], BF16),
            pltpu.VMEM((2, ny, 2, share, hidden), BF16),
            pltpu.VMEM((2, ny, share, hidden), BF16),
            pltpu.VMEM((2, ny, share, hidden), BF16),
            pltpu.VMEM((2, ny, half - 1, share, hidden), BF16),
            pltpu.VMEM((ny, share, hidden), F32),
            pltpu.VMEM((2, ny, 2, share, hidden), BF16),
            pltpu.VMEM((2, ny, t, width), F32),
            pltpu.VMEM((2, ny, nx - 1, t, width), BF16),
            pltpu.VMEM((2, ny, nx - 1, t, width), BF16),
            pltpu.VMEM((2, 2, ny, t, width), BF16),
            pltpu.VMEM((2, 2, nx - 1, t, width), BF16),
            pltpu.VMEM((2, ny, t, width), BF16),
            pltpu.SemaphoreType.DMA((6 + 2 * ny,)),
            dma(2, ny, nx - 1), dma(2, ny, nx - 1, PIECES), dma(2, 2, ny), dma(2, ny, PIECES),
            dma(2, 2, nx - 1), dma(2, 2, nx - 1, PIECES), dma(1), dma(2, ny, CHUNKS),
            dma(1), dma(2, ny, half - 1, CHUNKS), dma(1), dma(2, ny, CHUNKS),
            dma(2, ny, nx - 1), dma(2, ny, nx - 1, PIECES), dma(2, 2, ny), dma(2, 2, ny, PIECES),
            dma(2, 2, nx - 1), dma(2, 2, nx - 1, PIECES),
        ],
        compiler_params=pltpu.CompilerParams(
            collective_id=0, has_side_effects=True, vmem_limit_bytes=60 * 2**20
        ),
    )(tokens, grad_out, w_in, w_out)
    tok_all, grad_all = tok_all.reshape(-1, width), grad_all.reshape(-1, width)
    act_all, d_pre_all = act_all.reshape(-1, hidden), d_pre_all.reshape(-1, hidden)
    win_grad, wout_grad, mlp_out, tok_grad = finish(
        tok_all, d_pre_all, act_all, grad_all, mlp_out, tok_grad, scale
    )
    return mlp_out, tok_grad, win_grad, wout_grad


def solution(mesh):
    rows_spec = P(("gx", "gy"), "gz")
    in_spec = P("gz", ("gy", "gx"))
    out_spec = P(("gy", "gx"), "gz")
    sizes = (mesh.shape["gx"], mesh.shape["gy"], mesh.shape["gz"])
    return jax.shard_map(
        functools.partial(per_device, *sizes),
        mesh=mesh,
        in_specs=(rows_spec, rows_spec, in_spec, out_spec),
        out_specs=(rows_spec, rows_spec, in_spec, out_spec),
        check_vma=False,
    )
```

```python
import functools
import math

import jax
import jax.numpy as jnp
from jax import lax
from jax.experimental import pallas as pl
from jax.experimental.pallas import tpu as pltpu
from jax.sharding import PartitionSpec as P

MESH = pl.DeviceIdType.MESH
F32, BF16 = jnp.float32, jnp.bfloat16

GATHER_VIA = (False, True)
REDUCE_VIA = (True, False)
PIECES = 2
CHUNKS = 2
WIDE = 768
KINDS = "YZFCWTPJGEXR"
PLANS = (
    (
        1000, 1001, 2000, 2001, 3010, 1100, 2100, 5000, 2101, 4000, 4001, 3011, 4010, 3020,
        4100, 3021, 5100, 3030, 4011, 7010, 8010, 7000, 8000, 4020, 3031, 4021, 7020, 7011,
        7021, 1101, 8020, 8011, 9010, 4030, 3110, 3130, 4031, 8021, 3131, 6100, 7030, 7001,
        7031, 4101, 9020, 8030, 9011, 3120, 6101, 9000, 8031, 8001, 3111, 4130, 9021, 3121,
        4131, 10010, 7130, 10020, 7100, 7131, 12010, 9030, 10021, 8100, 10011, 4120, 9031, 8130,
        4121, 7120, 7101, 4110, 4111, 8131, 10030, 9001, 7110, 10031, 12020, 10000, 11000, 7111,
        10001, 7121, 8120, 12011, 6000, 8121, 8110, 11001, 9130, 9100, 9131, 12030, 6001, 12031,
        10130, 8111, 9120, 12021, 10131, 8101, 9121, 10120, 12130, 10121, 9110, 9111, 12131, 10110,
        12120, 9101, 10111, 10100, 12121, 10101, 12110, 12000, 12111, 12001, 12100, 12101,
    ),
    (
        1000, 1001, 2000, 2001, 3020, 3010, 3011, 3021, 4000, 5000, 3120, 3030, 3121, 4010,
        3031, 3130, 4011, 4001, 5100, 7010, 7000, 8010, 4020, 1100, 4021, 2100, 7020, 3131,
        2101, 8020, 4030, 1101, 7011, 8000, 7021, 9010, 3110, 8011, 4031, 6100, 7030, 7001,
        7031, 9020, 8021, 8030, 3111, 9000, 8031, 4130, 4120, 9011, 4100, 6101, 9021, 4131,
        8001, 4101, 10010, 7130, 10020, 7100, 4110, 7131, 10021, 10011, 9030, 9031, 4121, 8130,
        4111, 7120, 7101, 10030, 9001, 8131, 7110, 10031, 10000, 11000, 8120, 7111, 10001, 7121,
        8110, 6000, 12010, 8121, 9130, 11001, 9131, 6001, 9120, 10130, 8100, 10131, 8111, 12030,
        9110, 8101, 9121, 10120, 12031, 10121, 12011, 9111, 12020, 12000, 9100, 10110, 12130, 9101,
        10111, 10100, 12131, 12021, 10101, 12110, 12120, 12001, 12111, 12121, 12100, 12101,
    ),
)


def contract(left, right, dims):
    return lax.dot_general(left, right, (dims, ((), ())), preferred_element_type=F32)


def order_table(ny):
    centre = (ny - 1) / 2
    return [
        sorted(range(ny), key=lambda k: (abs(k - z), abs(k - centre))) for z in range(ny)
    ]


def schedule(ny):
    steps = [("W", 0, 0), ("W", 1, 0), ("T", 0, 0), ("T", 1, 0)]
    for arr in range(2):
        steps += [("Y", arr, 0), ("Z", arr, 0)]
        steps += [("F", arr, i) for i in range(1, ny)] + [("C", arr, i) for i in range(ny)]
        for name in "PJGE":
            steps += [(name, arr, i) for i in range(ny)]
        steps += [("X", arr, 0)]
    for arr in range(2):
        steps += [("R", arr, i) for i in reversed(range(ny))]
    steps = [(*step, p) for step in steps for p in range(PIECES) if step[0] != "W" or p == 0]
    plans = (steps, steps)
    if ny == 4:
        plans = [
            [
                (KINDS[step // 1000 - 1], step // 100 % 10, step // 10 % 10, step % 10)
                for step in plan
            ]
            for plan in PLANS
        ]
    cut = []
    for plan in plans:
        parts = [[]]
        for step in plan:
            if step[0] in "PET":
                parts += [step, []]
            else:
                parts[-1].append(step)
        cut.append(parts)
    out = []
    for ends, inside in zip(*cut):
        if ends == inside:
            out.append(([], [], [ends] if isinstance(ends, tuple) else ends))
        else:
            out.append((ends, inside, []))
    for arr in range(2):
        last = max(at for at, part in enumerate(out) if part[2] and part[2][0][:2] == ("E", arr))
        out.insert(last + 1, ([], [], [("S", arr, 0, 0)]))
    return out


def ring_kernel(
    nx, ny, nz,
    tok_ref, grad_ref, win_ref, wout_ref,
    mlp_ref, tgrad_ref, tok_out, grad_out, act_out, dpre_out,
    rows_all, win, wout, win_t, wout_t, part, pair_in, paired, part_in, slope, hid,
    mine_sum, cross, y_in, z_in, v_in, fold,
    local, *pairs,
):
    a_y, a_z, a_v, p_sem, b_sem, c_sem, d_y, d_z, d_v = zip(pairs[::2], pairs[1::2])
    x, y, z = lax.axis_index("gx"), lax.axis_index("gy"), lax.axis_index("gz")
    t, width = tok_ref.shape
    hidden = win_ref.shape[1]
    rows = nx * t
    share = rows // 2
    half = nz // 2
    chunks = CHUNKS if hidden % (128 * CHUNKS) == 0 else 1
    core, chip = lax.rem(z, 2), lax.div(z, 2)
    partner = z + 1 - 2 * core
    sends = {}

    def pick(values):
        total = 0
        for at, value in enumerate(values):
            total = total + jnp.where(y == at, value, 0)
        return total

    table = order_table(ny)
    near = [pick([table[at][i] for at in range(ny)]) for i in range(ny)]
    gap = [pick([abs(table[at][i] - at) for at in range(ny)]) for i in range(ny)]
    gaps = [{abs(table[at][i] - at) for at in range(ny)} for i in range(ny)]
    heading = [jnp.where(near[i] < y, 0, 1) for i in range(ny)]
    step_of = [1 - 2 * heading[i] for i in range(ny)]
    back = [1 - heading[i] for i in range(ny)]
    beyond = [
        jnp.logical_or(
            jnp.logical_and(near[i] < y, y < ny - 1), jnp.logical_and(near[i] > y, y > 0)
        )
        for i in range(ny)
    ]
    has_up, has_down = y < ny - 1, y > 0
    at_end = jnp.logical_or(y == 0, y == ny - 1)
    inside = jnp.logical_not(at_end)
    role = [None]

    def negate(pred):
        return (not pred) if isinstance(pred, bool) else jnp.logical_not(pred)

    def by_line_anywhere(flags, arr, i):
        if not flags[arr] or i == 0 or 1 not in gaps[i]:
            return False
        return True if gaps[i] == {1} else gap[i] == 1

    lines = {}
    for flags in (GATHER_VIA, REDUCE_VIA):
        for arr in range(2):
            for i in range(ny):
                found = by_line_anywhere(flags, arr, i)
                lines[flags, arr, i] = (found, negate(found))

    def via(flags, arr, i):
        if role[0] is None:
            return lines[flags, arr, i]
        here = abs(order_table(ny)[1 if role[0] == "inside" else 0][i] - (role[0] == "inside"))
        return (flags[arr] and here == 1), not (flags[arr] and here == 1)

    def onward(i):
        return {None: beyond[i], "end": False, "inside": True}[role[0]]

    def upward():
        return True if role[0] == "inside" else has_up

    def downward():
        return True if role[0] == "inside" else has_down

    def when(pred, body):
        if pred is True:
            body()
        elif pred is not False:
            pl.when(pred)(body)

    def remote(src, dst, leaving, landing, device):
        return pltpu.make_async_remote_copy(
            src_ref=src, dst_ref=dst, send_sem=leaving, recv_sem=landing,
            device_id=device, device_id_type=MESH,
        )

    def send(src, dst, sems, index, device, pred=lambda: True, leaving=None, bulk=None, key=None):
        now = pred()
        if now is False:
            return
        leaving = index[:-1] if leaving is None else leaving
        copy = remote(src, dst, sems[0].at[leaving], sems[1].at[index], device)
        when(now, copy.start)
        sends.setdefault(key, (sems, leaving, index, bulk, pred))

    def arrive(ref, sems, index):
        leaving = sems[0].at[(0,) * len(sems[0].shape)]
        remote(ref, ref, leaving, sems[1].at[index], {"gz": z}).wait_recv()

    def depart():
        for sems, leaving, index, bulk, pred in sends.values():
            ref = rows_all.at[0, 0, 0] if bulk is None else bulk
            copy = remote(ref, ref, sems[0].at[leaving], sems[1].at[index], {"gz": z})
            when(pred(), copy.wait_send)

    def peer(e):
        return {"gx": lax.rem(x + e, nx)}

    def piece(p):
        return pl.ds(p * (width // PIECES), width // PIECES)

    def chunk(c):
        return pl.ds(c * (hidden // chunks), hidden // chunks)

    def tiles(size, body, base=0, widest=256):
        tile = next(n for n in (widest, 256, 128) if size % n == 0)

        def step(i, carry):
            body(pl.ds(pl.multiple_of(base + i * tile, 128), tile))
            return carry

        lax.fori_loop(0, size // tile, step, 0)

    stage = [
        pltpu.make_async_copy(tok_ref, rows_all.at[0, y, 0], local.at[0]),
        pltpu.make_async_copy(grad_ref, rows_all.at[1, y, 0], local.at[1]),
        pltpu.make_async_copy(win_ref, win, local.at[2]),
        pltpu.make_async_copy(wout_ref, wout, local.at[3]),
    ]
    for copy in stage:
        copy.start()
    barrier = pltpu.get_barrier_semaphore()
    for name, me, n in (("gx", x, nx), ("gy", y, ny), ("gz", z, nz)):
        for d in range(1, n):
            pl.semaphore_signal(
                barrier, inc=1, device_id={name: lax.rem(me + d, n)}, device_id_type=MESH
            )
    pl.semaphore_wait(barrier, nx + ny + nz - 3)
    stores = []

    def to_columns(arr, i, p, pred=lambda: True):
        block = rows_all.at[arr, near[i], 0, :, piece(p)]
        for e in range(1, nx):
            dst = rows_all.at[arr, near[i], nx - e, :, piece(p)]
            send(
                block, dst, a_y, (arr, i, nx - e - 1, p), peer(e), pred, key=("a_y", arr, i, e)
            )

    def own_columns(arr, i, p):
        if p == 0:
            stage[arr].wait()
        to_columns(arr, 0, p)

    def own_line(arr, i, p):
        block = rows_all.at[arr, y, 0, :, piece(p)]
        for turn, to, pred in ((0, y + 1, upward), (1, y - 1, downward)):
            send(
                block, block, a_z, (arr, y, p), {"gy": to}, pred, (arr, turn, y),
                key=("a_z", arr, turn),
            )

    def own_column(arr, i, p):
        block = rows_all.at[arr, near[i], 0, :, piece(p)]
        arrive(block, a_z, (arr, near[i], p))
        send(
            block, block, a_z, (arr, near[i], p), {"gy": y + step_of[i]}, lambda: onward(i),
            (arr, heading[i], near[i]), key=("a_z", arr, i, 0),
        )
        to_columns(arr, i, p, lambda: via(GATHER_VIA, arr, i)[1])

    def other_columns(arr, i, p):
        by_line, by_column = via(GATHER_VIA, arr, i)
        for e in range(1, nx):
            block = rows_all.at[arr, near[i], e, :, piece(p)]
            when(by_line, lambda: arrive(block, a_v, (arr, heading[i], e - 1, p)))
            when(by_column, lambda: arrive(block, a_y, (arr, i, e - 1, p)))
            if i == 0 and GATHER_VIA[arr]:
                for turn, to, pred in ((0, y + 1, upward), (1, y - 1, downward)):
                    send(
                        block, block, a_v, (arr, turn, e - 1, p), {"gy": to}, pred,
                        key=("a_v", arr, turn, e),
                    )

    def turn_over(arr, i, p):
        src, dst = ((win, win_t), (wout, wout_t))[arr]
        side = src.shape[0] // PIECES
        tall = 256 if side % 256 == 0 else 128
        for j in range(side // tall):
            at = p * side + j * tall
            def body(cols):
                dst[cols, at:at + tall] = src[at:at + tall, cols].T
            tiles(src.shape[1], body)

    def project(arr, i, c):
        left = rows_all.at[arr, near[i]]

        def body(cols):
            lhs = left[...].reshape(rows, width)
            out = contract(lhs, (win, wout_t)[arr][:, cols], ((1,), (0,)))
            part[arr, i, :, :, cols] = out.astype(BF16).reshape(2, share, -1)

        tiles(hidden // chunks, body, c * (hidden // chunks), WIDE)
        send(
            part.at[arr, i, 1 - core, :, chunk(c)], pair_in.at[arr, i, :, chunk(c)],
            p_sem, (arr, i, c), {"gz": partner}, leaving=(0,), bulk=pair_in, key="p",
        )

    def join(arr, i, c):
        def body(cols):
            total = part[arr, i, core, :, cols].astype(F32)
            total = total + pair_in[arr, i, :, cols].astype(F32)
            paired[arr, i, :, cols] = total.astype(BF16)

        arrive(pair_in.at[arr, i, :, chunk(c)], p_sem, (arr, i, c))
        tiles(hidden // chunks, body, c * (hidden // chunks))
        for d in range(1, half):
            to = lax.rem(chip + d, half)
            send(
                paired.at[arr, i, :, chunk(c)], part_in.at[arr, i, d - 1, :, chunk(c)],
                b_sem, (arr, i, d - 1, c), {"gz": 2 * to + core}, leaving=(0,), bulk=part_in,
                key="b",
            )

    def activate(arr, i, c):
        def body(cols):
            total = paired[arr, i, :, cols].astype(F32)
            for d in range(1, half):
                total = total + part_in[arr, i, d - 1, :, cols].astype(F32)
            if arr == 0:
                cdf = 0.5 * (1.0 + lax.erf(total * 0.7071067811865476))
                density = jnp.exp(-0.5 * total * total) * 0.3989422804014327
                slope[i, :, cols] = cdf + total * density
                hid[arr, i, core, :, cols] = (total * cdf).astype(BF16)
            else:
                hid[arr, i, core, :, cols] = (total * slope[i, :, cols]).astype(BF16)

        for d in range(1, half):
            arrive(part_in.at[arr, i, d - 1, :, chunk(c)], b_sem, (arr, i, d - 1, c))
        tiles(hidden // chunks, body, c * (hidden // chunks))
        mine = hid.at[arr, i, core, :, chunk(c)]
        send(
            mine, mine, c_sem, (arr, i, c), {"gz": partner}, leaving=(0,), bulk=pair_in, key="c"
        )

    def expand(arr, i, p):
        if p == 0:
            for c in range(chunks):
                arrive(hid.at[arr, i, 1 - core, :, chunk(c)], c_sem, (arr, i, c))
        left = hid.at[arr, i]

        def body(cols):
            lhs = left[...].reshape(rows, hidden)
            out = contract(lhs, (wout, win_t)[arr][:, cols], ((1,), (0,)))
            mine_sum[arr, i, :, cols] = out[:t]
            for e in range(1, nx):
                cross[arr, i, e - 1, :, cols] = out[e * t:(e + 1) * t].astype(BF16)

        tiles(width // PIECES, body, p * (width // PIECES), WIDE)
        if i == 0 and REDUCE_VIA[arr]:
            return
        for e in range(1, nx):
            src = cross.at[arr, i, e - 1, :, piece(p)]
            send(
                src, v_in.at[arr, back[i], e - 1, :, piece(p)], d_v, (arr, back[i], e - 1, p),
                {"gy": y - step_of[i]}, lambda: via(REDUCE_VIA, arr, i)[0],
                key=("d_v", arr, i, e),
            )
            send(
                src, y_in.at[arr, i, nx - e - 1, :, piece(p)], d_y, (arr, i, nx - e - 1, p),
                peer(e), lambda: via(REDUCE_VIA, arr, i)[1], key=("d_y", arr, i, e),
            )

    def own_cross(arr, i, p):
        if not REDUCE_VIA[arr]:
            return
        for e in range(1, nx):
            for turn, pred in ((0, downward()), (1, upward())):
                def take(turn=turn):
                    got = v_in.at[arr, turn, e - 1, :, piece(p)]
                    arrive(got, d_v, (arr, turn, e - 1, p))

                    def body(cols):
                        total = cross[arr, 0, e - 1, :, cols].astype(F32)
                        total = total + v_in[arr, turn, e - 1, :, cols].astype(F32)
                        cross[arr, 0, e - 1, :, cols] = total.astype(BF16)

                    tiles(width // PIECES, body, p * (width // PIECES))

                when(pred, take)
            src = cross.at[arr, 0, e - 1, :, piece(p)]
            send(
                src, y_in.at[arr, 0, nx - e - 1, :, piece(p)], d_y, (arr, 0, nx - e - 1, p),
                peer(e), key=("d_y", arr, 0, e),
            )

    def reduce(arr, i, p):
        def from_columns():
            for e in range(1, nx):
                arrive(y_in.at[arr, i, e - 1, :, piece(p)], d_y, (arr, i, e - 1, p))

            def body(cols):
                total = mine_sum[arr, i, :, cols]
                for e in range(1, nx):
                    total = total + y_in[arr, i, e - 1, :, cols].astype(F32)
                mine_sum[arr, i, :, cols] = total

            tiles(width // PIECES, body, p * (width // PIECES))

        def from_line(turn, at):
            arrive(z_in.at[arr, turn, at, :, piece(p)], d_z, (arr, turn, at, p))

            def body(cols):
                total = mine_sum[arr, i, :, cols] + z_in[arr, turn, at, :, cols].astype(F32)
                mine_sum[arr, i, :, cols] = total

            tiles(width // PIECES, body, p * (width // PIECES))

        out = (mlp_ref, tgrad_ref)[arr]
        when(via(REDUCE_VIA, arr, i)[1], from_columns)
        if i == 0:
            when(downward(), lambda: from_line(0, y))
            when(upward(), lambda: from_line(1, y))
            out[:, piece(p)] = mine_sum[arr, 0, :, piece(p)].astype(BF16)
            return
        when(onward(i), lambda: from_line(back[i], near[i]))

        def body(cols):
            fold[arr, i, :, cols] = mine_sum[arr, i, :, cols].astype(BF16)

        tiles(width // PIECES, body, p * (width // PIECES))
        send(
            fold.at[arr, i, :, piece(p)], z_in.at[arr, back[i], near[i], :, piece(p)],
            d_z, (arr, back[i], near[i], p), {"gy": y - step_of[i]}, key=("d_z", arr, i),
        )

    def store(arr, i, p):
        stores.append(
            pltpu.make_async_copy(rows_all.at[arr], (tok_out, grad_out)[arr], local.at[4 + arr])
        )
        stores[-1].start()
        for i in range(ny):
            out = (act_out, dpre_out)[arr].at[near[i]]
            stores.append(pltpu.make_async_copy(hid.at[arr, i], out, local.at[6 + arr * ny + i]))
            stores[-1].start()

    acts = {
        "Y": own_columns, "Z": own_line, "F": own_column, "C": other_columns, "T": turn_over,
        "P": project, "J": join, "G": activate, "E": expand, "X": own_cross, "R": reduce,
        "S": store, "W": lambda arr, i, p: stage[2 + arr].wait(),
    }
    def run(steps):
        for name, arr, i, p in steps:
            if name not in "PJG" or p < chunks:
                acts[name](arr, i, p)

    def run_at(steps, place, pred):
        def body():
            role[0] = place
            run(steps)
            role[0] = None

        if steps:
            pl.when(pred)(body)

    for at_ends, insides, both in schedule(ny):
        run_at(at_ends, "end", at_end)
        run_at(insides, "inside", inside)
        run(both)
    depart()
    for copy in stores:
        copy.wait()


def grad_kernel(
    scale, tok_ref, dpre_ref, act_ref, grad_ref, mlp_ref, tgrad_ref,
    win_ref, wout_ref, mlp_out, tgrad_out,
    tok, dpre, act, grad, rows, win, wout, loads, stores,
):
    def load(src, dst, at):
        copy = pltpu.make_async_copy(src, dst, loads.at[at])
        copy.start()
        return copy

    first = [load(tok_ref, tok, 0), load(dpre_ref, dpre, 1)]

    def product(left, right, total, out, sem):
        tall = next(n for n in (256, 128) if total.shape[0] % n == 0)

        def step(i, carry):
            part = pl.ds(pl.multiple_of(i * tall, 128), tall)
            total[part, :] = contract(left[:, part], right[...], ((0,), (0,))) * scale
            pltpu.make_async_copy(total.at[part, :], out.at[part, :], sem).start()
            return carry

        count = total.shape[0] // tall
        lax.fori_loop(0, count, step, 0, unroll=2 if count % 2 == 0 else 1)

    for copy in first:
        copy.wait()
    second = [load(act_ref, act, 2), load(grad_ref, grad, 3)]
    passing = [load(mlp_ref, rows.at[0], 4), load(tgrad_ref, rows.at[1], 5)]
    product(tok, dpre, win, win_ref, stores.at[0])
    for copy in second:
        copy.wait()
    product(act, grad, wout, wout_ref, stores.at[1])
    for at, out in enumerate((mlp_out, tgrad_out)):
        passing[at].wait()
        pltpu.make_async_copy(rows.at[at], out, stores.at[2 + at]).start()
    pltpu.make_async_copy(win, win_ref, stores.at[0]).wait()
    pltpu.make_async_copy(wout, wout_ref, stores.at[1]).wait()
    for at, out in enumerate((mlp_out, tgrad_out)):
        pltpu.make_async_copy(rows.at[at], out, stores.at[2 + at]).wait()


def finish(tok, dpre, act, grad, mlp, tgrad, scale):
    tokens, width = tok.shape
    hidden = dpre.shape[1]
    shape = jax.ShapeDtypeStruct
    anywhere = pl.BlockSpec(memory_space=pl.ANY)
    return pl.pallas_call(
        functools.partial(grad_kernel, scale),
        out_shape=(
            shape((width, hidden), F32), shape((hidden, width), F32),
            shape(mlp.shape, BF16), shape(tgrad.shape, BF16),
        ),
        in_specs=[anywhere] * 6,
        out_specs=(anywhere,) * 4,
        scratch_shapes=[
            pltpu.VMEM(tok.shape, BF16), pltpu.VMEM(dpre.shape, BF16),
            pltpu.VMEM(act.shape, BF16), pltpu.VMEM(grad.shape, BF16),
            pltpu.VMEM((2, *mlp.shape), BF16),
            pltpu.VMEM((width, hidden), F32), pltpu.VMEM((hidden, width), F32),
            pltpu.SemaphoreType.DMA((6,)), pltpu.SemaphoreType.DMA((4,)),
        ],
        compiler_params=pltpu.CompilerParams(vmem_limit_bytes=60 * 2**20),
        cost_estimate=pl.CostEstimate(
            flops=4 * tokens * width * hidden, transcendentals=0,
            bytes_accessed=8 * width * hidden + 4 * tokens * (width + hidden),
        ),
    )(tok, dpre, act, grad, mlp, tgrad)


def per_device(nx, ny, nz, tokens, grad_out, w_in, w_out):
    t, width = tokens.shape
    hidden = w_in.shape[1]
    rows = nx * t
    share = rows // 2
    half = nz // 2
    scale = 1.0 / math.sqrt(ny * t)
    anywhere = pl.BlockSpec(memory_space=pl.ANY)
    vmem = pl.BlockSpec(memory_space=pltpu.VMEM)
    dma = lambda *shape: pltpu.SemaphoreType.DMA(shape)
    shape = jax.ShapeDtypeStruct
    mlp_out, tok_grad, tok_all, grad_all, act_all, d_pre_all = pl.pallas_call(
        functools.partial(ring_kernel, nx, ny, nz),
        out_shape=(
            shape((t, width), BF16), shape((t, width), BF16),
            shape((ny, nx, t, width), BF16), shape((ny, nx, t, width), BF16),
            shape((ny, 2, share, hidden), BF16), shape((ny, 2, share, hidden), BF16),
        ),
        in_specs=[anywhere] * 4,
        out_specs=(vmem, vmem, anywhere, anywhere, anywhere, anywhere),
        scratch_shapes=[
            pltpu.VMEM((2, ny, nx, t, width), BF16),
            pltpu.VMEM(w_in.shape, BF16),
            pltpu.VMEM(w_out.shape, BF16),
            pltpu.VMEM(w_in.shape[::-1], BF16),
            pltpu.VMEM(w_out.shape[::-1], BF16),
            pltpu.VMEM((2, ny, 2, share, hidden), BF16),
            pltpu.VMEM((2, ny, share, hidden), BF16),
            pltpu.VMEM((2, ny, share, hidden), BF16),
            pltpu.VMEM((2, ny, half - 1, share, hidden), BF16),
            pltpu.VMEM((ny, share, hidden), F32),
            pltpu.VMEM((2, ny, 2, share, hidden), BF16),
            pltpu.VMEM((2, ny, t, width), F32),
            pltpu.VMEM((2, ny, nx - 1, t, width), BF16),
            pltpu.VMEM((2, ny, nx - 1, t, width), BF16),
            pltpu.VMEM((2, 2, ny, t, width), BF16),
            pltpu.VMEM((2, 2, nx - 1, t, width), BF16),
            pltpu.VMEM((2, ny, t, width), BF16),
            pltpu.SemaphoreType.DMA((6 + 2 * ny,)),
            dma(2, ny, nx - 1), dma(2, ny, nx - 1, PIECES), dma(2, 2, ny), dma(2, ny, PIECES),
            dma(2, 2, nx - 1), dma(2, 2, nx - 1, PIECES), dma(1), dma(2, ny, CHUNKS),
            dma(1), dma(2, ny, half - 1, CHUNKS), dma(1), dma(2, ny, CHUNKS),
            dma(2, ny, nx - 1), dma(2, ny, nx - 1, PIECES), dma(2, 2, ny), dma(2, 2, ny, PIECES),
            dma(2, 2, nx - 1), dma(2, 2, nx - 1, PIECES),
        ],
        compiler_params=pltpu.CompilerParams(
            collective_id=0, has_side_effects=True, vmem_limit_bytes=60 * 2**20
        ),
    )(tokens, grad_out, w_in, w_out)
    tok_all, grad_all = tok_all.reshape(-1, width), grad_all.reshape(-1, width)
    act_all, d_pre_all = act_all.reshape(-1, hidden), d_pre_all.reshape(-1, hidden)
    win_grad, wout_grad, mlp_out, tok_grad = finish(
        tok_all, d_pre_all, act_all, grad_all, mlp_out, tok_grad, scale
    )
    return mlp_out, tok_grad, win_grad, wout_grad


def solution(mesh):
    rows_spec = P(("gx", "gy"), "gz")
    in_spec = P("gz", ("gy", "gx"))
    out_spec = P(("gy", "gx"), "gz")
    sizes = (mesh.shape["gx"], mesh.shape["gy"], mesh.shape["gz"])
    return jax.shard_map(
        functools.partial(per_device, *sizes),
        mesh=mesh,
        in_specs=(rows_spec, rows_spec, in_spec, out_spec),
        out_specs=(rows_spec, rows_spec, in_spec, out_spec),
        check_vma=False,
    )
```
